16 devices in a mesh: dp: 4 (over z, y), tp: 4 (over x, core).
Axes of the slice: x: 2, y: 2, z: 2, core: 2. Of those that a mesh axis runs over, the one named last changes fastest.
Arguments:
- tok_hidden: bfloat16 [256, 1536], P('dp'), parts along dimension 0
- seq_lens: int32 [256], P('dp'), parts along dimension 0
- k_cache: bfloat16 [256, 512, 4, 128], P('dp', None, 'tp'), parts along dimension 0
- v_cache: bfloat16 [256, 512, 4, 128], P('dp', None, 'tp'), parts along dimension 0
- next_tok: int32 [256], P('dp'), parts along dimension 0
- g_attn: bfloat16 [1536], replicated
- w_q: bfloat16 [1536, 1536], P(None, 'tp')
- b_q: bfloat16 [1536], P('tp')
- w_k: bfloat16 [1536, 512], P(None, 'tp')
- b_k: bfloat16 [512], P('tp')
- w_v: bfloat16 [1536, 512], P(None, 'tp')
- b_v: bfloat16 [512], P('tp')
- w_o: bfloat16 [1536, 1536], P('tp')
- g_mlp: bfloat16 [1536], replicated
- w_gate: bfloat16 [1536, 8960], P(None, 'tp')
- w_up: bfloat16 [1536, 8960], P(None, 'tp')
- w_down: bfloat16 [8960, 1536], P('tp')
- g_final: bfloat16 [1536], replicated
- w_head: bfloat16 [151936, 1536], P('tp')
Outputs:
- output 1: bfloat16 [256, 1536], P('dp'), parts along dimension 0
- output 2: bfloat16 [256, 512, 4, 128], P('dp', None, 'tp'), parts along dimension 0
- output 3: bfloat16 [256, 512, 4, 128], P('dp', None, 'tp'), parts along dimension 0
- output 4: float32 [256], P('dp'), parts along dimension 0
- output 5: float32 [256], P('dp'), parts along dimension 0
There are 4 independent parts. The reference program is written for one: setup_inputs(seed, part) draws one part's arguments, and reference() takes and returns one part's arrays. A program takes and returns all parts, laid end to end along the dimension named above; an argument that names none is the same for every part.
All inputs are finite; a program needn't handle non-finite values.
Results may differ from the reference program's by a relative error of at most 0.0126328.
Values are sent between devices in bfloat16 or wider.
A program may use at most 1 GiB of HBM per device.

```python
import math
import jax
import jax.numpy as jnp
from jax import lax

BATCH = 64
LMAX = 512
D = 1536
HEADS = 12
KV_HEADS = 2
HEAD = 128
FF = 8960
VOCAB = 151936
KV_SLOTS = 4
THETA = 1000000
EPS = 1e-6
COPIES = KV_SLOTS // KV_HEADS
GROUP = HEADS // KV_SLOTS


def rms_norm(values, gain_vec):
    vals_f32 = values.astype(jnp.float32)
    inv_rms = lax.rsqrt(jnp.mean(vals_f32 * vals_f32, axis=-1, keepdims=True) + EPS)
    return (vals_f32 * inv_rms * gain_vec.astype(jnp.float32)).astype(jnp.bfloat16)


def rotary(values, positions):
    half_dim = values.shape[-1] // 2
    inv_freq = jnp.power(float(THETA), jnp.arange(half_dim, dtype=jnp.float32) * (-2.0 / values.shape[-1]))
    angles = positions.astype(jnp.float32)[:, None] * inv_freq[None, :]
    cos_part = jnp.cos(angles)[:, None, :]
    sin_part = jnp.sin(angles)[:, None, :]
    first_half = values[..., :half_dim]
    second_half = values[..., half_dim:]
    return jnp.concatenate([first_half * cos_part - second_half * sin_part, second_half * cos_part + first_half * sin_part], axis=-1)


def draw_lengths(len_key):
    exp_key, off_key, pick_key = jax.random.split(len_key, 3)
    log_max = int(math.log2(LMAX))
    exponent = jax.random.randint(exp_key, (BATCH,), 0, log_max)
    base_len = jnp.left_shift(jnp.ones((BATCH,), jnp.int32), exponent)
    offset = jax.random.randint(off_key, (BATCH,), 0, LMAX) % base_len
    longest = jax.random.randint(pick_key, (), 0, BATCH)
    return jnp.where(jnp.arange(BATCH) == longest, LMAX - 1, base_len + offset).astype(jnp.int32)


def gaussian(rand_key, arr_shape, spread):
    return jax.random.normal(rand_key, arr_shape, jnp.float32) * spread


def setup_inputs(seed: int = 0, part: int = 0) -> dict:
    shared_keys = jax.random.split(jax.random.key(seed), 16)
    part_keys = jax.random.split(jax.random.fold_in(jax.random.key(seed + 1), part), 8)
    k_scale = math.sqrt(max(math.log(LMAX / 8.0), 1.0) / 1.25)
    k_base = gaussian(part_keys[2], (BATCH, LMAX, KV_HEADS, HEAD), k_scale)
    v_base = gaussian(part_keys[3], (BATCH, LMAX, KV_HEADS, HEAD), 1.0)
    w_k = gaussian(shared_keys[3], (D, KV_HEADS, HEAD), D ** -0.5)
    b_k = gaussian(shared_keys[4], (KV_HEADS, HEAD), 0.5)
    w_v = gaussian(shared_keys[5], (D, KV_HEADS, HEAD), D ** -0.5)
    b_v = gaussian(shared_keys[6], (KV_HEADS, HEAD), 0.5)
    return {
        'tok_hidden': gaussian(part_keys[0], (BATCH, D), 1.0).astype(jnp.bfloat16),
        'seq_lens': draw_lengths(part_keys[1]),
        'k_cache': jnp.repeat(k_base, COPIES, axis=2).astype(jnp.bfloat16),
        'v_cache': jnp.repeat(v_base, COPIES, axis=2).astype(jnp.bfloat16),
        'next_tok': jax.random.randint(part_keys[4], (BATCH,), 0, VOCAB),
        'g_attn': (1.0 + gaussian(shared_keys[0], (D,), 0.2)).astype(jnp.bfloat16),
        'w_q': gaussian(shared_keys[1], (D, HEADS * HEAD), D ** -0.5).astype(jnp.bfloat16),
        'b_q': gaussian(shared_keys[2], (HEADS * HEAD,), 0.5).astype(jnp.bfloat16),
        'w_k': jnp.repeat(w_k, COPIES, axis=1).reshape(D, KV_SLOTS * HEAD).astype(jnp.bfloat16),
        'b_k': jnp.repeat(b_k, COPIES, axis=0).reshape(KV_SLOTS * HEAD).astype(jnp.bfloat16),
        'w_v': jnp.repeat(w_v, COPIES, axis=1).reshape(D, KV_SLOTS * HEAD).astype(jnp.bfloat16),
        'b_v': jnp.repeat(b_v, COPIES, axis=0).reshape(KV_SLOTS * HEAD).astype(jnp.bfloat16),
        'w_o': gaussian(shared_keys[7], (HEADS * HEAD, D), (HEADS * HEAD) ** -0.5).astype(jnp.bfloat16),
        'g_mlp': (1.0 + gaussian(shared_keys[8], (D,), 0.2)).astype(jnp.bfloat16),
        'w_gate': gaussian(shared_keys[9], (D, FF), D ** -0.5).astype(jnp.bfloat16),
        'w_up': gaussian(shared_keys[10], (D, FF), D ** -0.5).astype(jnp.bfloat16),
        'w_down': gaussian(shared_keys[11], (FF, D), FF ** -0.5).astype(jnp.bfloat16),
        'g_final': (3.0 + gaussian(shared_keys[12], (D,), 0.5)).astype(jnp.bfloat16),
        'w_head': gaussian(shared_keys[13], (VOCAB, D), D ** -0.5).astype(jnp.bfloat16),
    }


def reference(tok_hidden, seq_lens, k_cache, v_cache, next_tok, g_attn, w_q, b_q, w_k, b_k, w_v, b_v, w_o, g_mlp, w_gate, w_up, w_down, g_final, w_head):
    normed = rms_norm(tok_hidden, g_attn)
    q_proj = jnp.dot(normed, w_q, preferred_element_type=jnp.float32) + b_q.astype(jnp.float32)
    k_proj = jnp.dot(normed, w_k, preferred_element_type=jnp.float32) + b_k.astype(jnp.float32)
    v_proj = jnp.dot(normed, w_v, preferred_element_type=jnp.float32) + b_v.astype(jnp.float32)
    q_rot = rotary(q_proj.reshape(BATCH, HEADS, HEAD), seq_lens).astype(jnp.bfloat16)
    k_new = rotary(k_proj.reshape(BATCH, KV_SLOTS, HEAD), seq_lens).astype(jnp.bfloat16)
    v_new = v_proj.reshape(BATCH, KV_SLOTS, HEAD).astype(jnp.bfloat16)
    slot_ids = jnp.arange(LMAX)
    write_mask = (slot_ids[None, :] == seq_lens[:, None])[:, :, None, None]
    k_all = jnp.where(write_mask, k_new[:, None], k_cache)
    v_all = jnp.where(write_mask, v_new[:, None], v_cache)

    def one_row(row_args):
        q_row, k_row, v_row, length = row_args
        q_grp = q_row.reshape(KV_SLOTS, GROUP, HEAD).astype(jnp.float32)
        scores = jnp.einsum('kgd,lkd->kgl', q_grp, k_row.astype(jnp.float32)) * (HEAD ** -0.5)
        scores = jnp.where((slot_ids <= length)[None, None, :], scores, -jnp.inf)
        attn_probs = jax.nn.softmax(scores, axis=-1).astype(jnp.bfloat16).astype(jnp.float32)
        attn_vals = jnp.einsum('kgl,lkd->kgd', attn_probs, v_row.astype(jnp.float32))
        return attn_vals.reshape(HEADS * HEAD).astype(jnp.bfloat16)

    attn_out = lax.map(one_row, (q_rot, k_all, v_all, seq_lens))
    attn_proj = jnp.dot(attn_out, w_o, preferred_element_type=jnp.float32)
    residual = (tok_hidden.astype(jnp.float32) + attn_proj).astype(jnp.bfloat16)
    mlp_in = rms_norm(residual, g_mlp)
    gate_proj = jnp.dot(mlp_in, w_gate, preferred_element_type=jnp.float32)
    up_proj = jnp.dot(mlp_in, w_up, preferred_element_type=jnp.float32)
    hidden = (jax.nn.silu(gate_proj) * up_proj).astype(jnp.bfloat16)
    down_proj = jnp.dot(hidden, w_down, preferred_element_type=jnp.float32)
    y_out = (residual.astype(jnp.float32) + down_proj).astype(jnp.bfloat16)
    final_norm = rms_norm(y_out, g_final)
    logits = lax.dot_general(final_norm, w_head, (((1,), (1,)), ((), ())), preferred_element_type=jnp.float32)
    norm_lse = jax.nn.logsumexp(logits, axis=-1)
    vocab_ids = jnp.arange(VOCAB)
    target = jnp.sum(jnp.where(vocab_ids[None, :] == next_tok[:, None], logits, 0.0), axis=-1)
    tok_logp = target - norm_lse
    return (y_out, k_all, v_all, tok_logp, norm_lse)
```

```python
import functools
import math
import jax
import jax.numpy as jnp
import numpy as np
from jax import lax
from jax.experimental import pallas as pl
from jax.experimental.pallas import tpu as pltpu
from jax.sharding import PartitionSpec as P

THETA = 1000000.0
EPS = 1e-6
MESH = pl.DeviceIdType.MESH
F32 = jnp.float32
BF16 = jnp.bfloat16

B = 64
L = 512
D = 1536
HD = 128
G = 3
FF = 2240
VOC = 37984
NDP = 4
NTP = 4
NB = 8
NCH = B // NB
VQ = VOC // NDP
VC = 528
NVC = 18
HALF = B // 2
FF_CHUNKS = ((0, 512), (512, 512), (1024, 512), (1536, 512), (2048, 192))
NT = (((1,), (1,)), ((), ()))
NN = (((1,), (0,)), ((), ()))


def _dot(a, b, dims):
    return lax.dot_general(a, b, dims, preferred_element_type=F32)


def _row(ref, n):
    vals = ref[...].astype(F32)
    return jnp.concatenate([vals[i:i + 1, :] for i in range(n)], axis=1)


def _rms(vals, gain):
    inv = lax.rsqrt(jnp.mean(vals * vals, axis=-1, keepdims=True) + EPS)
    return (vals * inv * gain).astype(BF16)


def attn_kernel(lens_s, x_ref, lens_ref, g_ref, bq_ref, bk_ref, bv_ref, freq_ref, wq_h, wk_h, wv_h, wo_h, k_h, v_h,
                part_ref, ko_h, vo_h,
                wq, wk, wv, wo, kbuf, vbuf, q_sc, kn_sc, vn_sc, len_sc, o_sc, wsem, ksem, vsem, kosem, vosem):
    def wcopy(i):
        src, dst = ((wq_h, wq), (wk_h, wk), (wv_h, wv), (wo_h, wo))[i]
        return pltpu.make_async_copy(src, dst, wsem.at[i])

    def rows(c):
        return pl.ds(pl.multiple_of(c * NB, NB), NB)

    def kin(c):
        return pltpu.make_async_copy(k_h.at[rows(c)], kbuf.at[rows(c)], ksem.at[c])

    def vin(c):
        return pltpu.make_async_copy(v_h.at[rows(c)], vbuf.at[rows(c)], vsem.at[c])

    def kout(c):
        return pltpu.make_async_copy(kbuf.at[rows(c)], ko_h.at[rows(c)], kosem.at[c])

    def vout(c):
        return pltpu.make_async_copy(vbuf.at[rows(c)], vo_h.at[rows(c)], vosem.at[c])

    for i in range(3):
        wcopy(i).start()
    for c in range(NCH):
        kin(c).start()
        vin(c).start()
    wcopy(3).start()

    normed = _rms(x_ref[...].astype(F32), _row(g_ref, D // 128))
    r_id = lax.broadcasted_iota(jnp.int32, (B, B), 0)
    c_id = lax.broadcasted_iota(jnp.int32, (B, B), 1)
    len_f = jnp.broadcast_to(lens_ref[...].astype(F32), (B, B))
    len_col = jnp.sum(jnp.where(r_id == c_id, len_f, 0.0), axis=1, keepdims=True)
    len_full = jnp.broadcast_to(len_col, (B, HD))
    len_sc[...] = len_full
    angles = len_full * freq_ref[...]
    cos = jnp.cos(angles)
    lane = lax.broadcasted_iota(jnp.int32, (B, HD), 1)
    sin = jnp.where(lane < HD // 2, -1.0, 1.0) * jnp.sin(angles)

    def rope(vals):
        out = vals * cos + pltpu.roll(vals, HD // 2, 1) * sin
        return out.astype(BF16).astype(F32)

    wcopy(0).wait()
    q_all = _dot(normed, wq[...], NN) + _row(bq_ref, G)
    for h in range(G):
        q_sc[h] = rope(q_all[:, h * HD:(h + 1) * HD])
    wcopy(1).wait()
    kn_sc[...] = rope(_dot(normed, wk[...], NN) + bk_ref[...].astype(F32))
    wcopy(2).wait()
    vn_sc[...] = (_dot(normed, wv[...], NN) + bv_ref[...].astype(F32)).astype(BF16).astype(F32)

    scale = HD ** -0.5
    sub16 = lax.broadcasted_iota(jnp.int32, (16, HD), 0)
    col_id = lax.broadcasted_iota(jnp.int32, (G * NB, L), 1).astype(F32)
    row_s = lax.broadcasted_iota(jnp.int32, (G * NB, L), 0) % NB
    row_o = lax.broadcasted_iota(jnp.int32, (G * NB, HD), 0) % NB

    def chunk(c, carry):
        r0 = pl.multiple_of(c * NB, NB)
        kin(c).wait()
        vin(c).wait()
        for b in range(NB):
            row = r0 + b
            length = lens_s[row]
            base = pl.multiple_of((length // 16) * 16, 16)
            hit = sub16 == length - base
            for buf, new in ((kbuf, kn_sc), (vbuf, vn_sc)):
                old = buf[row, pl.ds(base, 16), :].astype(F32)
                fresh = jnp.broadcast_to(new[pl.ds(row, 1), :], (16, HD))
                buf[row, pl.ds(base, 16), :] = jnp.where(hit, fresh, old).astype(BF16)
        q8 = jnp.concatenate([q_sc[h, pl.ds(r0, NB), :] for h in range(G)], axis=0).astype(BF16)
        scores = jnp.zeros((G * NB, L), F32)
        for b in range(NB):
            scores = jnp.where(row_s == b, _dot(q8, kbuf[r0 + b], NT), scores)
        len8 = len_sc[pl.ds(r0, NB), :]
        len24 = jnp.concatenate([len8] * G, axis=0)
        keep = col_id <= jnp.concatenate([len24] * (L // HD), axis=1)
        scores = jnp.where(keep, scores * scale, -jnp.inf)
        top = jnp.max(scores, axis=1, keepdims=True)
        exps = jnp.exp(scores - top)
        probs = (exps / jnp.sum(exps, axis=1, keepdims=True)).astype(BF16)
        out = jnp.zeros((G * NB, HD), F32)
        for b in range(NB):
            out = jnp.where(row_o == b, _dot(probs, vbuf[r0 + b], NN), out)
        for h in range(G):
            o_sc[pl.ds(r0, NB), h * HD:(h + 1) * HD] = out[h * NB:(h + 1) * NB, :]
        kout(c).start()
        vout(c).start()
        return carry

    lax.fori_loop(0, NCH, chunk, 0)
    wcopy(3).wait()
    part_ref[...] = _dot(o_sc[...].astype(BF16), wo[...], NN).astype(BF16)

    def drain(c, carry):
        kout(c).wait()
        vout(c).wait()
        return carry

    lax.fori_loop(0, NCH, drain, 0)


def attention(x, lens, k_cache, v_cache, g_attn, w_q, b_q, w_k, b_k, w_v, b_v, w_o):
    inv_freq = np.power(THETA, np.arange(HD // 2, dtype=np.float64) * (-2.0 / HD)).astype(np.float32)
    freq = jnp.asarray(np.concatenate([inv_freq, inv_freq])[None, :])
    vmem = pl.BlockSpec(memory_space=pltpu.VMEM)
    smem = pl.BlockSpec(memory_space=pltpu.SMEM)
    hbm = pl.BlockSpec(memory_space=pltpu.HBM)
    return pl.pallas_call(
        attn_kernel,
        name='attn',
        out_shape=(
            jax.ShapeDtypeStruct((B, D), BF16),
            jax.ShapeDtypeStruct((B, L, HD), BF16),
            jax.ShapeDtypeStruct((B, L, HD), BF16),
        ),
        in_specs=[smem] + [vmem] * 7 + [hbm] * 6,
        out_specs=(vmem, hbm, hbm),
        scratch_shapes=[
            pltpu.VMEM((D, G * HD), BF16),
            pltpu.VMEM((D, HD), BF16),
            pltpu.VMEM((D, HD), BF16),
            pltpu.VMEM((G * HD, D), BF16),
            pltpu.VMEM((B, L, HD), BF16),
            pltpu.VMEM((B, L, HD), BF16),
            pltpu.VMEM((G, B, HD), F32),
            pltpu.VMEM((B, HD), F32),
            pltpu.VMEM((B, HD), F32),
            pltpu.VMEM((B, HD), F32),
            pltpu.VMEM((B, G * HD), F32),
            pltpu.SemaphoreType.DMA((4,)),
            pltpu.SemaphoreType.DMA((NCH,)),
            pltpu.SemaphoreType.DMA((NCH,)),
            pltpu.SemaphoreType.DMA((NCH,)),
            pltpu.SemaphoreType.DMA((NCH,)),
        ],
        compiler_params=pltpu.CompilerParams(vmem_limit_bytes=40 * 1024 * 1024),
        cost_estimate=pl.CostEstimate(flops=400_000_000, bytes_accessed=37_000_000, transcendentals=0),
    )(lens, x, lens.reshape(1, B), g_attn.reshape(D // 128, 128), b_q.reshape(G, 128), b_k.reshape(1, 128),
      b_v.reshape(1, 128), freq, w_q, w_k, w_v, w_o, k_cache, v_cache)


def tail_kernel(part_ref, x_ref, gm_ref, gf_ref, tok_ref, wg_h, wu_h, wd_h, wh_h,
                y_ref, logp_ref, lse_ref,
                wg, wu, wd, wh, r1, ps, r2, abuf, h_sc, dpart, r3, ps2, r4, fall, toks, st_out, st_in,
                gsem, usem, dsem, hsem, send, recv, st_send, st_recv):
    dp = lax.axis_index('dp')
    tp = lax.axis_index('tp')
    core = tp % 2
    sib = tp + 1 - 2 * core
    xpeer = (tp + 2) % 4
    me = dp * NTP + tp
    ydp = dp + 1 - 2 * (dp % 2)
    zdp = (dp + 2) % 4
    ddp = (ydp + 2) % 4
    mine = pl.ds(pl.multiple_of(core * HALF, HALF), HALF)
    other = pl.ds(pl.multiple_of((1 - core) * HALF, HALF), HALF)

    def gcopy(i):
        s = pl.ds(*FF_CHUNKS[i])
        return pltpu.make_async_copy(wg_h.at[s], wg.at[s], gsem.at[i])

    def ucopy(i):
        s = pl.ds(*FF_CHUNKS[i])
        return pltpu.make_async_copy(wu_h.at[s], wu.at[s], usem.at[i])

    dcopy = pltpu.make_async_copy(wd_h, wd, dsem.at[0])
    v0 = dp * VQ - 8 * (dp // 3)

    def hcopy(j):
        src = wh_h.at[pl.ds(pl.multiple_of(v0 + j * VC, 8), VC)]
        return pltpu.make_async_copy(src, wh.at[pl.ds(pl.multiple_of(j * VC, VC), VC)], hsem.at[j])

    def remote(src, dst, i, **where):
        return pltpu.make_async_remote_copy(src_ref=src, dst_ref=dst, send_sem=send.at[i], recv_sem=recv.at[i],
                                            device_id=where, device_id_type=MESH)

    for i in range(len(FF_CHUNKS)):
        gcopy(i).start()
        ucopy(i).start()
    dcopy.start()

    tok2 = jnp.concatenate([tok_ref[...], tok_ref[...]], axis=1)
    toks[dp] = jnp.broadcast_to(tok2, (8, 128))

    barrier = pltpu.get_barrier_semaphore()
    for k in range(1, NDP * NTP):
        there = (me + k) % (NDP * NTP)
        pl.semaphore_signal(barrier, inc=1, device_id={'dp': there // NTP, 'tp': there % NTP}, device_id_type=MESH)
    pl.semaphore_wait(barrier, NDP * NTP - 1)

    c0 = remote(part_ref.at[other], r1, 0, tp=sib)
    c0.start()
    tok_copies = [remote(toks.at[dp], toks.at[dp], 13 + i, dp=d) for i, d in enumerate((ydp, zdp, ddp))]
    for c in tok_copies:
        c.start()
    c0.wait()
    ps[...] = (part_ref[mine, :].astype(F32) + r1[...].astype(F32)).astype(BF16)
    c1 = remote(ps, r2, 1, tp=xpeer)
    c1.start()
    gain_m = _row(gm_ref, D // 128)
    gain_f = _row(gf_ref, D // 128)
    c1.wait()
    a_half = (x_ref[mine, :].astype(F32) + (ps[...].astype(F32) + r2[...].astype(F32))).astype(BF16)
    abuf[mine, :] = a_half
    c2 = remote(abuf.at[mine], abuf.at[mine], 2, tp=sib)
    c2.start()
    c2.wait()

    mlp_in = _rms(abuf[...].astype(F32), gain_m)
    for i, (s, n) in enumerate(FF_CHUNKS):
        gcopy(i).wait()
        gate = _dot(mlp_in, wg[s:s + n, :], NT)
        ucopy(i).wait()
        up = _dot(mlp_in, wu[s:s + n, :], NT)
        h_sc[:, s:s + n] = (gate * (1.0 / (1.0 + jnp.exp(-gate))) * up).astype(BF16)
    dcopy.wait()
    for j in range(NVC):
        hcopy(j).start()
    dpart[...] = _dot(h_sc[...], wd[...], NN).astype(BF16)

    c3 = remote(dpart.at[other], r3, 3, tp=sib)
    c3.start()
    c3.wait()
    ps2[...] = (dpart[mine, :].astype(F32) + r3[...].astype(F32)).astype(BF16)
    c4 = remote(ps2, r4, 4, tp=xpeer)
    c4.start()
    c4.wait()
    y_half = (abuf[mine, :].astype(F32) + (ps2[...].astype(F32) + r4[...].astype(F32))).astype(BF16)
    y_ref[mine, :] = y_half

    def frows(d, c):
        return pl.ds(pl.multiple_of(d * B + c * HALF, HALF), HALF)

    own = frows(dp, core)
    fall[own, :] = _rms(y_half.astype(F32), gain_f)
    gathers = [remote(fall.at[own], fall.at[own], 7 + i, dp=d) for i, d in enumerate((ydp, zdp, ddp))]
    for c in gathers:
        c.start()
    c6 = remote(fall.at[own], fall.at[own], 6, tp=sib)
    c6.start()
    c5 = remote(y_ref.at[mine], y_ref.at[mine], 5, tp=sib)
    c5.start()
    forwards = []
    for i, d in enumerate((ydp, zdp, ddp)):
        gathers[i].wait_recv()
        fwd = remote(fall.at[frows(d, core)], fall.at[frows(d, core)], 10 + i, tp=sib)
        fwd.start()
        forwards.append(fwd)
    for c in tok_copies:
        c.wait()
    lane = lax.broadcasted_iota(jnp.int32, (8, 128), 1)
    lo = jnp.where(lane < B, toks[0], toks[1])
    hi = jnp.where(lane < B, toks[2], toks[3])
    want = jnp.concatenate([lo, hi], axis=1) - (tp * VOC + v0)
    first = 8 * (dp // 3)
    want = jnp.where((want >= first) & (want < first + VQ), want, -1)
    for c in gathers:
        c.wait_send()
    for c in forwards + [c5, c6]:
        c.wait()

    sub = lax.broadcasted_iota(jnp.int32, (VC // 8, 8, NDP * B), 0) * 8 + lax.broadcasted_iota(
        jnp.int32, (VC // 8, 8, NDP * B), 1)

    def vocab(j, carry):
        top, total, target = carry
        hcopy(j).wait()
        z = _dot(wh[pl.ds(pl.multiple_of(j * VC, VC), VC), :], fall[...], NT)
        drop_first = (first > 0) & (j == 0)
        drop_last = (first == 0) & (j == NVC - 1)
        z = jnp.concatenate([
            jnp.where(drop_first, -jnp.inf, z[:8]), z[8:VC - 8], jnp.where(drop_last, -jnp.inf, z[VC - 8:])], axis=0)
        z = z.reshape(VC // 8, 8, NDP * B)
        new_top = jnp.maximum(top, jnp.max(z, axis=0))
        total = total * jnp.exp(top - new_top) + jnp.sum(jnp.exp(z - new_top[None]), axis=0)
        hit = sub == (want - j * VC)[None]
        target = target + jnp.sum(jnp.where(hit, z, 0.0), axis=0)
        return new_top, total, target

    top, total, target = lax.fori_loop(0, NVC, vocab, (
        jnp.full((8, NDP * B), -jnp.inf, F32), jnp.zeros((8, NDP * B), F32), jnp.zeros((8, NDP * B), F32)))

    t_row = jnp.max(top, axis=0, keepdims=True)
    s_row = jnp.sum(total * jnp.exp(top - t_row), axis=0, keepdims=True)
    z_row = jnp.sum(target, axis=0, keepdims=True)
    row8 = lax.broadcasted_iota(jnp.int32, (8, NDP * B), 0)
    stats = jnp.where(row8 == 0, t_row, jnp.where(row8 == 1, s_row, z_row))
    st_out[0] = stats[:, :128]
    st_out[1] = stats[:, 128:]
    st_in[me] = jnp.where(dp // 2 == 0, stats[:, :128], stats[:, 128:])
    st_copies = []
    for k in range(1, NDP * NTP):
        there = (me + k) % (NDP * NTP)
        c = pltpu.make_async_remote_copy(
            src_ref=st_out.at[there // NTP // 2], dst_ref=st_in.at[me], send_sem=st_send.at[k],
            recv_sem=st_recv.at[k], device_id={'dp': there // NTP, 'tp': there % NTP}, device_id_type=MESH)
        c.start()
        st_copies.append(c)
    for c in st_copies:
        c.wait()
    every = st_in[...]
    tops = every[:, 0:1, :]
    best = jnp.max(tops, axis=0)
    mass = jnp.sum(every[:, 1:2, :] * jnp.exp(tops - best[None]), axis=0)
    hits = jnp.sum(every[:, 2:3, :], axis=0)
    lse = best + jnp.log(mass)
    logp = hits - lse
    left = dp % 2 == 0
    lse_ref[...] = jnp.where(left, lse[:, :B], lse[:, B:])
    logp_ref[...] = jnp.where(left, logp[:, :B], logp[:, B:])


def tail(part, x, g_mlp, g_final, next_tok, w_gate, w_up, w_down, w_head):
    vmem = pl.BlockSpec(memory_space=pltpu.VMEM)
    hbm = pl.BlockSpec(memory_space=pltpu.HBM)
    nff = len(FF_CHUNKS)
    half = pltpu.VMEM((HALF, D), BF16)
    return pl.pallas_call(
        tail_kernel,
        name='tail',
        out_shape=(
            jax.ShapeDtypeStruct((B, D), BF16),
            jax.ShapeDtypeStruct((1, B), F32),
            jax.ShapeDtypeStruct((1, B), F32),
        ),
        in_specs=[vmem] * 5 + [hbm] * 4,
        out_specs=(vmem, vmem, vmem),
        scratch_shapes=[
            pltpu.VMEM((FF, D), BF16),
            pltpu.VMEM((FF, D), BF16),
            pltpu.VMEM((FF, D), BF16),
            pltpu.VMEM((VC * NVC, D), BF16),
            half, half, half,
            pltpu.VMEM((B, D), BF16),
            pltpu.VMEM((B, FF), BF16),
            pltpu.VMEM((B, D), BF16),
            half, half, half,
            pltpu.VMEM((NDP * B, D), BF16),
            pltpu.VMEM((NDP, 8, 128), jnp.int32),
            pltpu.VMEM((2, 8, 128), F32),
            pltpu.VMEM((NDP * NTP, 8, 128), F32),
            pltpu.SemaphoreType.DMA((nff,)),
            pltpu.SemaphoreType.DMA((nff,)),
            pltpu.SemaphoreType.DMA((1,)),
            pltpu.SemaphoreType.DMA((NVC,)),
            pltpu.SemaphoreType.DMA((16,)),
            pltpu.SemaphoreType.DMA((16,)),
            pltpu.SemaphoreType.DMA((16,)),
            pltpu.SemaphoreType.DMA((16,)),
        ],
        compiler_params=pltpu.CompilerParams(
            vmem_limit_bytes=61 * 1024 * 1024, collective_id=0, has_side_effects=True),
        cost_estimate=pl.CostEstimate(flops=10_000_000_000, bytes_accessed=50_000_000, transcendentals=0),
    )(part, x, g_mlp.reshape(D // 128, 128), g_final.reshape(D // 128, 128), next_tok.reshape(1, B),
      w_gate.T, w_up.T, w_down, w_head)


def local_step(tok_hidden, seq_lens, k_cache, v_cache, next_tok, g_attn, w_q, b_q, w_k, b_k, w_v, b_v, w_o, g_mlp,
               w_gate, w_up, w_down, g_final, w_head):
    part, k_all, v_all = attention(
        tok_hidden, seq_lens, k_cache.reshape(B, L, HD), v_cache.reshape(B, L, HD), g_attn, w_q, b_q, w_k, b_k, w_v,
        b_v, w_o)
    y_out, tok_logp, norm_lse = tail(part, tok_hidden, g_mlp, g_final, next_tok, w_gate, w_up, w_down, w_head)
    return (y_out, k_all.reshape(B, L, 1, HD), v_all.reshape(B, L, 1, HD), tok_logp.reshape(B), norm_lse.reshape(B))


def solution(mesh):
    row_spec = P('dp', None)
    vec_spec = P('dp')
    cache_spec = P('dp', None, 'tp', None)
    col_spec = P(None, 'tp')
    part_spec = P('tp')
    whole_spec = P(None)
    in_specs = (row_spec, vec_spec, cache_spec, cache_spec, vec_spec, whole_spec, col_spec, part_spec, col_spec,
                part_spec, col_spec, part_spec, P('tp', None), whole_spec, col_spec, col_spec, P('tp', None),
                whole_spec, P('tp', None))
    out_specs = (row_spec, cache_spec, cache_spec, vec_spec, vec_spec)
    return jax.shard_map(local_step, mesh=mesh, in_specs=in_specs, out_specs=out_specs, check_vma=False)
```

```python
import functools
import math
import jax
import jax.numpy as jnp
import numpy as np
from jax import lax
from jax.experimental import pallas as pl
from jax.experimental.pallas import tpu as pltpu
from jax.sharding import PartitionSpec as P

THETA = 1000000.0
EPS = 1e-6
MESH = pl.DeviceIdType.MESH
F32 = jnp.float32
BF16 = jnp.bfloat16

B = 64
L = 512
D = 1536
HD = 128
G = 3
FF = 2240
VOC = 37984
NDP = 4
NTP = 4
NB = 8
NCH = B // NB
AHEAD = 3
VQ = VOC // NDP
VC = 528
NVC = 18
UNROLL = 6
HALF = B // 2
FF_CHUNKS = ((0, 512), (512, 512), (1024, 512), (1536, 512), (2048, 192))
NT = (((1,), (1,)), ((), ()))
NN = (((1,), (0,)), ((), ()))


def _dot(a, b, dims):
    return lax.dot_general(a, b, dims, preferred_element_type=F32)


def _row(ref, n):
    vals = ref[...].astype(F32)
    return jnp.concatenate([vals[i:i + 1, :] for i in range(n)], axis=1)


def _rms(vals, gain):
    inv = lax.rsqrt(jnp.mean(vals * vals, axis=-1, keepdims=True) + EPS)
    return (vals * inv * gain).astype(BF16)


def attn_kernel(x_h, lens_h, g_h, bq_h, bk_h, bv_h, freq_h, wq_h, wk_h, wv_h, wo_h, k_h, v_h,
                part_ref, ko_h, vo_h,
                lens_s, x_ref, lens_ref, g_ref, bq_ref, bk_ref, bv_ref, freq_ref,
                wq, wk, wv, wo, kbuf, vbuf, q_sc, kn_sc, vn_sc, len_sc, o_sc, isem, wsem, ksem, vsem, kosem, vosem):
    small = [pltpu.make_async_copy(src, dst, isem.at[i]) for i, (src, dst) in enumerate((
        (x_h, x_ref), (g_h, g_ref), (lens_h, lens_ref), (freq_h, freq_ref), (bq_h, bq_ref), (bk_h, bk_ref),
        (bv_h, bv_ref), (lens_h, lens_s)))]

    def wcopy(i):
        src, dst = ((wq_h, wq), (wk_h, wk), (wv_h, wv), (wo_h, wo))[i]
        return pltpu.make_async_copy(src, dst, wsem.at[i])

    def rows(c):
        return pl.ds(pl.multiple_of(c * NB, NB), NB)

    def kin(c):
        return pltpu.make_async_copy(k_h.at[rows(c)], kbuf.at[rows(c)], ksem.at[c])

    def vin(c):
        return pltpu.make_async_copy(v_h.at[rows(c)], vbuf.at[rows(c)], vsem.at[c])

    def kout(c):
        return pltpu.make_async_copy(kbuf.at[rows(c)], ko_h.at[rows(c)], kosem.at[c])

    def vout(c):
        return pltpu.make_async_copy(vbuf.at[rows(c)], vo_h.at[rows(c)], vosem.at[c])

    with jax.named_scope('starts'):
        for c in small:
            c.start()
        for i in range(3):
            wcopy(i).start()
        for c in range(AHEAD):
            kin(c).start()
            vin(c).start()

    with jax.named_scope('qkv'):
        for c in small:
            c.wait()
        normed = _rms(x_ref[...].astype(F32), _row(g_ref, D // 128))
        r_id = lax.broadcasted_iota(jnp.int32, (B, B), 0)
        c_id = lax.broadcasted_iota(jnp.int32, (B, B), 1)
        len_f = jnp.broadcast_to(lens_ref[...].astype(F32), (B, B))
        len_col = jnp.sum(jnp.where(r_id == c_id, len_f, 0.0), axis=1, keepdims=True)
        len_full = jnp.broadcast_to(len_col, (B, HD))
        len_sc[...] = len_full
        angles = len_full * freq_ref[...]
        cos = jnp.cos(angles)
        lane = lax.broadcasted_iota(jnp.int32, (B, HD), 1)
        sin = jnp.where(lane < HD // 2, -1.0, 1.0) * jnp.sin(angles)

        def rope(vals):
            out = vals * cos + pltpu.roll(vals, HD // 2, 1) * sin
            return out.astype(BF16).astype(F32)

        wcopy(0).wait()
        q_all = _dot(normed, wq[...], NN) + _row(bq_ref, G)
        for h in range(G):
            q_sc[h] = rope(q_all[:, h * HD:(h + 1) * HD])
        wcopy(1).wait()
        kn_sc[...] = rope(_dot(normed, wk[...], NN) + bk_ref[...].astype(F32))
        wcopy(2).wait()
        vn_sc[...] = (_dot(normed, wv[...], NN) + bv_ref[...].astype(F32)).astype(BF16).astype(F32)

    scale = HD ** -0.5
    sub16 = lax.broadcasted_iota(jnp.int32, (16, HD), 0)
    col_id = lax.broadcasted_iota(jnp.int32, (G * NB, L), 1).astype(F32)
    row_s = lax.broadcasted_iota(jnp.int32, (G * NB, L), 0) % NB
    row_o = lax.broadcasted_iota(jnp.int32, (G * NB, HD), 0) % NB

    def chunk(c, carry):
        r0 = pl.multiple_of(c * NB, NB)
        kin(c).wait()
        vin(c).wait()

        @pl.when(c + AHEAD < NCH)
        def _():
            kin(c + AHEAD).start()
            vin(c + AHEAD).start()

        @pl.when(c + AHEAD == NCH)
        def _():
            wcopy(3).start()

        for b in range(NB):
            row = r0 + b
            length = lens_s[0, row]
            base = pl.multiple_of((length // 16) * 16, 16)
            hit = sub16 == length - base
            for buf, new in ((kbuf, kn_sc), (vbuf, vn_sc)):
                old = buf[row, pl.ds(base, 16), :].astype(F32)
                fresh = jnp.broadcast_to(new[pl.ds(row, 1), :], (16, HD))
                buf[row, pl.ds(base, 16), :] = jnp.where(hit, fresh, old).astype(BF16)
        q8 = jnp.concatenate([q_sc[h, pl.ds(r0, NB), :] for h in range(G)], axis=0).astype(BF16)
        scores = jnp.zeros((G * NB, L), F32)
        for b in range(NB):
            scores = jnp.where(row_s == b, _dot(q8, kbuf[r0 + b], NT), scores)
        len8 = len_sc[pl.ds(r0, NB), :]
        len24 = jnp.concatenate([len8] * G, axis=0)
        keep = col_id <= jnp.concatenate([len24] * (L // HD), axis=1)
        scores = jnp.where(keep, scores * scale, -jnp.inf)
        top = jnp.max(scores, axis=1, keepdims=True)
        exps = jnp.exp(scores - top)
        probs = (exps / jnp.sum(exps, axis=1, keepdims=True)).astype(BF16)
        out = jnp.zeros((G * NB, HD), F32)
        for b in range(NB):
            out = jnp.where(row_o == b, _dot(probs, vbuf[r0 + b], NN), out)
        for h in range(G):
            o_sc[pl.ds(r0, NB), h * HD:(h + 1) * HD] = out[h * NB:(h + 1) * NB, :]
        kout(c).start()
        vout(c).start()
        return carry

    with jax.named_scope('cache'):
        lax.fori_loop(0, NCH, chunk, 0)
    with jax.named_scope('proj'):
        wcopy(3).wait()
        part_ref[...] = _dot(o_sc[...].astype(BF16), wo[...], NN).astype(BF16)

    def drain(c, carry):
        kout(c).wait()
        vout(c).wait()
        return carry

    with jax.named_scope('drain'):
        lax.fori_loop(0, NCH, drain, 0)


def attention(x, lens, k_cache, v_cache, g_attn, w_q, b_q, w_k, b_k, w_v, b_v, w_o):
    inv_freq = np.power(THETA, np.arange(HD // 2, dtype=np.float64) * (-2.0 / HD)).astype(np.float32)
    freq = jnp.asarray(np.concatenate([inv_freq, inv_freq])[None, :])
    vmem = pl.BlockSpec(memory_space=pltpu.VMEM)
    hbm = pl.BlockSpec(memory_space=pltpu.HBM)
    return pl.pallas_call(
        attn_kernel,
        name='attn',
        out_shape=(
            jax.ShapeDtypeStruct((B, D), BF16),
            jax.ShapeDtypeStruct((B, L, HD), BF16),
            jax.ShapeDtypeStruct((B, L, HD), BF16),
        ),
        in_specs=[hbm] * 13,
        out_specs=(vmem, hbm, hbm),
        scratch_shapes=[
            pltpu.SMEM((1, B), jnp.int32),
            pltpu.VMEM((B, D), BF16),
            pltpu.VMEM((1, B), jnp.int32),
            pltpu.VMEM((D // 128, 128), BF16),
            pltpu.VMEM((G, 128), BF16),
            pltpu.VMEM((1, 128), BF16),
            pltpu.VMEM((1, 128), BF16),
            pltpu.VMEM((1, 128), F32),
            pltpu.VMEM((D, G * HD), BF16),
            pltpu.VMEM((D, HD), BF16),
            pltpu.VMEM((D, HD), BF16),
            pltpu.VMEM((G * HD, D), BF16),
            pltpu.VMEM((B, L, HD), BF16),
            pltpu.VMEM((B, L, HD), BF16),
            pltpu.VMEM((G, B, HD), F32),
            pltpu.VMEM((B, HD), F32),
            pltpu.VMEM((B, HD), F32),
            pltpu.VMEM((B, HD), F32),
            pltpu.VMEM((B, G * HD), F32),
            pltpu.SemaphoreType.DMA((8,)),
            pltpu.SemaphoreType.DMA((4,)),
            pltpu.SemaphoreType.DMA((NCH,)),
            pltpu.SemaphoreType.DMA((NCH,)),
            pltpu.SemaphoreType.DMA((NCH,)),
            pltpu.SemaphoreType.DMA((NCH,)),
        ],
        compiler_params=pltpu.CompilerParams(vmem_limit_bytes=62 * 1024 * 1024),
        cost_estimate=pl.CostEstimate(flops=400_000_000, bytes_accessed=37_000_000, transcendentals=0),
    )(x, lens.reshape(1, B), g_attn.reshape(D // 128, 128), b_q.reshape(G, 128), b_k.reshape(1, 128),
      b_v.reshape(1, 128), freq, w_q, w_k, w_v, w_o, k_cache, v_cache)


def tail_kernel(part_h, x_h, gm_h, gf_h, tok_h, wg_h, wu_h, wd_h, wh_h,
                y_h, st_in,
                part_ref, x_ref, gm_ref, gf_ref, tok_ref, y_ref, wg, wu, wd, wh, r1, ps, r2, abuf, h_sc, dpart, r3, ps2, r4, fall, toks, st_out,
                isem, gsem, usem, dsem, hsem, send, recv, st_send, st_recv):
    dp = lax.axis_index('dp')
    tp = lax.axis_index('tp')
    core = tp % 2
    sib = tp + 1 - 2 * core
    xpeer = (tp + 2) % 4
    me = dp * NTP + tp
    ydp = dp + 1 - 2 * (dp % 2)
    zdp = (dp + 2) % 4
    ddp = (ydp + 2) % 4
    mine = pl.ds(pl.multiple_of(core * HALF, HALF), HALF)
    other = pl.ds(pl.multiple_of((1 - core) * HALF, HALF), HALF)

    def gcopy(i):
        s = pl.ds(*FF_CHUNKS[i])
        return pltpu.make_async_copy(wg_h.at[s], wg.at[s], gsem.at[i])

    def ucopy(i):
        s = pl.ds(*FF_CHUNKS[i])
        return pltpu.make_async_copy(wu_h.at[s], wu.at[s], usem.at[i])

    dcopy = pltpu.make_async_copy(wd_h, wd, dsem.at[0])
    v0 = dp * VQ - 8 * (dp // 3)

    def hcopy(j):
        src = wh_h.at[pl.ds(pl.multiple_of(v0 + j * VC, 8), VC)]
        return pltpu.make_async_copy(src, wh.at[pl.ds(pl.multiple_of(j * VC, VC), VC)], hsem.at[j])

    def remote(src, dst, i, **where):
        return pltpu.make_async_remote_copy(src_ref=src, dst_ref=dst, send_sem=send.at[i], recv_sem=recv.at[i],
                                            device_id=where, device_id_type=MESH)

    small = [pltpu.make_async_copy(src, dst, isem.at[i]) for i, (src, dst) in enumerate((
        (part_h, part_ref), (tok_h, tok_ref), (x_h, x_ref), (gm_h, gm_ref), (gf_h, gf_ref)))]
    y_out = pltpu.make_async_copy(y_ref, y_h, isem.at[5])
    barrier = pltpu.get_barrier_semaphore()
    for k in range(1, NDP * NTP):
        there = (me + k) % (NDP * NTP)
        pl.semaphore_signal(barrier, inc=1, device_id={'dp': there // NTP, 'tp': there % NTP}, device_id_type=MESH)
    for c in small:
        c.start()
    gcopy(0).start()
    for c in small:
        c.wait()
    ucopy(0).start()
    for i in range(1, len(FF_CHUNKS)):
        gcopy(i).start()
        ucopy(i).start()
    dcopy.start()

    tok2 = jnp.concatenate([tok_ref[...], tok_ref[...]], axis=1)
    toks[dp] = jnp.broadcast_to(tok2, (8, 128))

    with jax.named_scope('barrier'):
        pl.semaphore_wait(barrier, NDP * NTP - 1)

    with jax.named_scope('sum1'):
        c0 = remote(part_ref.at[other], r1, 0, tp=sib)
        c0.start()
        tok_copies = [remote(toks.at[dp], toks.at[dp], 13 + i, dp=d) for i, d in enumerate((ydp, zdp, ddp))]
        for c in tok_copies:
            c.start()
        c0.wait()
        ps[...] = (part_ref[mine, :].astype(F32) + r1[...].astype(F32)).astype(BF16)
        c1 = remote(ps, r2, 1, tp=xpeer)
        c1.start()
        gain_m = _row(gm_ref, D // 128)
        gain_f = _row(gf_ref, D // 128)
        c1.wait()
        a_half = (x_ref[mine, :].astype(F32) + (ps[...].astype(F32) + r2[...].astype(F32))).astype(BF16)
        abuf[mine, :] = a_half
        c2 = remote(abuf.at[mine], abuf.at[mine], 2, tp=sib)
        c2.start()
        c2.wait()

    with jax.named_scope('mlp'):
        mlp_in = _rms(abuf[...].astype(F32), gain_m)
        for i in range(len(FF_CHUNKS)):
            gcopy(i).wait()
            ucopy(i).wait()
        dcopy.wait()
        for j in range(NVC):
            hcopy(j).start()
        for s, n in FF_CHUNKS:
            gate = _dot(mlp_in, wg[s:s + n, :], NT)
            up = _dot(mlp_in, wu[s:s + n, :], NT)
            h_sc[:, s:s + n] = (gate * (1.0 / (1.0 + jnp.exp(-gate))) * up).astype(BF16)
        dpart[...] = _dot(h_sc[...], wd[...], NN).astype(BF16)

    with jax.named_scope('sum2'):
        c3 = remote(dpart.at[other], r3, 3, tp=sib)
        c3.start()
        c3.wait()
        ps2[...] = (dpart[mine, :].astype(F32) + r3[...].astype(F32)).astype(BF16)
        c4 = remote(ps2, r4, 4, tp=xpeer)
        c4.start()
        c4.wait()
        y_half = (abuf[mine, :].astype(F32) + (ps2[...].astype(F32) + r4[...].astype(F32))).astype(BF16)
        y_ref[mine, :] = y_half

    def frows(d, c):
        return pl.ds(pl.multiple_of(d * B + c * HALF, HALF), HALF)

    with jax.named_scope('gather'):
        own = frows(dp, core)
        fall[own, :] = _rms(y_half.astype(F32), gain_f)
        gathers = [remote(fall.at[own], fall.at[own], 7 + i, dp=d) for i, d in enumerate((ydp, zdp, ddp))]
        for c in gathers:
            c.start()
        c6 = remote(fall.at[own], fall.at[own], 6, tp=sib)
        c6.start()
        c5 = remote(y_ref.at[mine], y_ref.at[mine], 5, tp=sib)
        c5.start()
        forwards = []
        for i, d in enumerate((ydp, zdp, ddp)):
            gathers[i].wait_recv()
            fwd = remote(fall.at[frows(d, core)], fall.at[frows(d, core)], 10 + i, tp=sib)
            fwd.start()
            forwards.append(fwd)
        for c in tok_copies:
            c.wait()
        lane = lax.broadcasted_iota(jnp.int32, (8, 128), 1)
        lo = jnp.where(lane < B, toks[0], toks[1])
        hi = jnp.where(lane < B, toks[2], toks[3])
        want = jnp.concatenate([lo, hi], axis=1) - (tp * VOC + v0)
        first = 8 * (dp // 3)
        want = jnp.where((want >= first) & (want < first + VQ), want, -1)
        for c in gathers:
            c.wait_send()
        for c in forwards + [c5, c6]:
            c.wait()
        y_out.start()
        for j in range(NVC):
            hcopy(j).wait()

    sub = lax.broadcasted_iota(jnp.int32, (VC // 8, 8, NDP * B), 0) * 8 + lax.broadcasted_iota(
        jnp.int32, (VC // 8, 8, NDP * B), 1)

    def vocab(j, carry):
        top, total, target = carry
        z = _dot(wh[pl.ds(pl.multiple_of(j * VC, VC), VC), :], fall[...], NT)
        drop_first = (first > 0) & (j == 0)
        drop_last = (first == 0) & (j == NVC - 1)
        z = jnp.concatenate([
            jnp.where(drop_first, -jnp.inf, z[:8]), z[8:VC - 8], jnp.where(drop_last, -jnp.inf, z[VC - 8:])], axis=0)
        z = z.reshape(VC // 8, 8, NDP * B)
        new_top = jnp.maximum(top, jnp.max(z, axis=0))
        total = total * jnp.exp(top - new_top) + jnp.sum(jnp.exp(z - new_top[None]), axis=0)
        hit = sub == (want - j * VC)[None]
        target = target + jnp.sum(jnp.where(hit, z, 0.0), axis=0)
        return new_top, total, target

    with jax.named_scope('head'):
        def several(i, carry):
            for k in range(UNROLL):
                carry = vocab(i * UNROLL + k, carry)
            return carry

        top, total, target = lax.fori_loop(0, NVC // UNROLL, several, (
            jnp.full((8, NDP * B), -jnp.inf, F32), jnp.zeros((8, NDP * B), F32), jnp.zeros((8, NDP * B), F32)))

    with jax.named_scope('stats'):
        t_row = jnp.max(top, axis=0, keepdims=True)
        s_row = jnp.sum(total * jnp.exp(top - t_row), axis=0, keepdims=True)
        z_row = jnp.sum(target, axis=0, keepdims=True)
        row8 = lax.broadcasted_iota(jnp.int32, (8, NDP * B), 0)
        stats = jnp.where(row8 == 0, t_row, jnp.where(row8 == 1, s_row, z_row))
        st_out[0] = stats[:, :128]
        st_out[1] = stats[:, 128:]
        st_in[me] = jnp.where(dp // 2 == 0, stats[:, :128], stats[:, 128:])
        st_copies = []
        for k in range(1, NDP * NTP):
            there = (me + k) % (NDP * NTP)
            c = pltpu.make_async_remote_copy(
                src_ref=st_out.at[there // NTP // 2], dst_ref=st_in.at[me], send_sem=st_send.at[k],
                recv_sem=st_recv.at[k], device_id={'dp': there // NTP, 'tp': there % NTP}, device_id_type=MESH)
            c.start()
            st_copies.append(c)
        for c in st_copies:
            c.wait()
        y_out.wait()


def finish_kernel(y_in, stats_h, y_ref, logp_ref, lse_ref, ybuf, stats_ref, sem):
    get_y = pltpu.make_async_copy(y_in, ybuf, sem.at[0])
    put_y = pltpu.make_async_copy(ybuf, y_ref, sem.at[1])
    get_stats = pltpu.make_async_copy(stats_h, stats_ref, sem.at[2])
    get_y.start()
    get_stats.start()
    get_y.wait()
    put_y.start()
    get_stats.wait()
    every = stats_ref[...]
    best = jnp.max(every[:, 0:1, :], axis=0)
    mass = jnp.sum(every[:, 1:2, :] * jnp.exp(every[:, 0:1, :] - best[None]), axis=0)
    hits = jnp.sum(every[:, 2:3, :], axis=0)
    lse = best + jnp.log(mass)
    logp = hits - lse
    left = lax.axis_index('dp') % 2 == 0
    lse_ref[...] = jnp.where(left, lse[:, :B], lse[:, B:])
    logp_ref[...] = jnp.where(left, logp[:, :B], logp[:, B:])
    put_y.wait()


def tail(part, x, g_mlp, g_final, next_tok, w_gate, w_up, w_down, w_head):
    vmem = pl.BlockSpec(memory_space=pltpu.VMEM)
    hbm = pl.BlockSpec(memory_space=pltpu.HBM)
    nff = len(FF_CHUNKS)
    half = pltpu.VMEM((HALF, D), BF16)
    y, stats = pl.pallas_call(
        tail_kernel,
        name='tail',
        out_shape=(
            jax.ShapeDtypeStruct((B, D), BF16),
            jax.ShapeDtypeStruct((NDP * NTP, 8, 128), F32),
        ),
        in_specs=[hbm] * 9,
        out_specs=(hbm, vmem),
        scratch_shapes=[
            pltpu.VMEM((B, D), BF16),
            pltpu.VMEM((B, D), BF16),
            pltpu.VMEM((D // 128, 128), BF16),
            pltpu.VMEM((D // 128, 128), BF16),
            pltpu.VMEM((1, B), jnp.int32),
            pltpu.VMEM((B, D), BF16),
            pltpu.VMEM((FF, D), BF16),
            pltpu.VMEM((FF, D), BF16),
            pltpu.VMEM((FF, D), BF16),
            pltpu.VMEM((VC * NVC, D), BF16),
            half, half, half,
            pltpu.VMEM((B, D), BF16),
            pltpu.VMEM((B, FF), BF16),
            pltpu.VMEM((B, D), BF16),
            half, half, half,
            pltpu.VMEM((NDP * B, D), BF16),
            pltpu.VMEM((NDP, 8, 128), jnp.int32),
            pltpu.VMEM((2, 8, 128), F32),
            pltpu.SemaphoreType.DMA((6,)),
            pltpu.SemaphoreType.DMA((nff,)),
            pltpu.SemaphoreType.DMA((nff,)),
            pltpu.SemaphoreType.DMA((1,)),
            pltpu.SemaphoreType.DMA((NVC,)),
            pltpu.SemaphoreType.DMA((16,)),
            pltpu.SemaphoreType.DMA((16,)),
            pltpu.SemaphoreType.DMA((16,)),
            pltpu.SemaphoreType.DMA((16,)),
        ],
        compiler_params=pltpu.CompilerParams(
            vmem_limit_bytes=61 * 1024 * 1024, collective_id=0, has_side_effects=True),
        cost_estimate=pl.CostEstimate(flops=10_000_000_000, bytes_accessed=50_000_000, transcendentals=0),
    )(part, x, g_mlp.reshape(D // 128, 128), g_final.reshape(D // 128, 128), next_tok.reshape(1, B),
      w_gate.T, w_up.T, w_down, w_head)
    return pl.pallas_call(
        finish_kernel,
        name='finish',
        out_shape=(
            jax.ShapeDtypeStruct((B, D), BF16),
            jax.ShapeDtypeStruct((1, B), F32),
            jax.ShapeDtypeStruct((1, B), F32),
        ),
        in_specs=[hbm] * 2,
        out_specs=(hbm, vmem, vmem),
        scratch_shapes=[
            pltpu.VMEM((B, D), BF16),
            pltpu.VMEM((NDP * NTP, 8, 128), F32),
            pltpu.SemaphoreType.DMA((3,)),
        ],
        compiler_params=pltpu.CompilerParams(vmem_limit_bytes=62 * 1024 * 1024),
    )(y, stats)


def local_step(tok_hidden, seq_lens, k_cache, v_cache, next_tok, g_attn, w_q, b_q, w_k, b_k, w_v, b_v, w_o, g_mlp,
               w_gate, w_up, w_down, g_final, w_head):
    part, k_all, v_all = attention(
        tok_hidden, seq_lens, k_cache.reshape(B, L, HD), v_cache.reshape(B, L, HD), g_attn, w_q, b_q, w_k, b_k, w_v,
        b_v, w_o)
    y_out, tok_logp, norm_lse = tail(part, tok_hidden, g_mlp, g_final, next_tok, w_gate, w_up, w_down, w_head)
    return (y_out, k_all.reshape(B, L, 1, HD), v_all.reshape(B, L, 1, HD), tok_logp.reshape(B), norm_lse.reshape(B))


def solution(mesh):
    row_spec = P('dp', None)
    vec_spec = P('dp')
    cache_spec = P('dp', None, 'tp', None)
    col_spec = P(None, 'tp')
    part_spec = P('tp')
    whole_spec = P(None)
    in_specs = (row_spec, vec_spec, cache_spec, cache_spec, vec_spec, whole_spec, col_spec, part_spec, col_spec,
                part_spec, col_spec, part_spec, P('tp', None), whole_spec, col_spec, col_spec, P('tp', None),
                whole_spec, P('tp', None))
    out_specs = (row_spec, cache_spec, cache_spec, vec_spec, vec_spec)
    return jax.shard_map(local_step, mesh=mesh, in_specs=in_specs, out_specs=out_specs, check_vma=False)
```

```python
import functools
import math
import jax
import jax.numpy as jnp
import numpy as np
from jax import lax
from jax.experimental import pallas as pl
from jax.experimental.pallas import tpu as pltpu
from jax.sharding import PartitionSpec as P

THETA = 1000000.0
EPS = 1e-6
MESH = pl.DeviceIdType.MESH
F32 = jnp.float32
BF16 = jnp.bfloat16

B = 64
L = 512
D = 1536
HD = 128
G = 3
FF = 2240
VOC = 37984
NDP = 4
NTP = 4
NB = 8
NCH = B // NB
AHEAD = 3
VQ = VOC // NDP
VC = 528
NVC = 18
UNROLL = 6
HALF = B // 2
FF_CHUNKS = ((0, 512), (512, 512), (1024, 512), (1536, 512), (2048, 192))
NT = (((1,), (1,)), ((), ()))
NN = (((1,), (0,)), ((), ()))


def _dot(a, b, dims):
    return lax.dot_general(a, b, dims, preferred_element_type=F32)


def in_hbm(*arrays):
    return [pltpu.with_memory_space_constraint(a, pltpu.HBM) for a in arrays]


def in_vmem(*arrays):
    return [pltpu.with_memory_space_constraint(a, pltpu.VMEM) for a in arrays]


def _row(ref, n):
    vals = ref[...].astype(F32)
    return jnp.concatenate([vals[i:i + 1, :] for i in range(n)], axis=1)


def _rms(vals, gain):
    inv = lax.rsqrt(jnp.mean(vals * vals, axis=-1, keepdims=True) + EPS)
    return (vals * inv * gain).astype(BF16)


def attn_kernel(x_h, lens_h, g_h, bq_h, bk_h, bv_h, freq_h, gm_h, gf_h, tok_h, wq_h, wk_h, wv_h, wo_h, k_h, v_h,
                part_ref, kbuf, vbuf, x_ref, gm_ref, gf_ref, tok_ref,
                lens_s, lens_ref, g_ref, bq_ref, bk_ref, bv_ref, freq_ref,
                wq, wk, wv, wo, q_sc, kn_sc, vn_sc, len_sc, o_sc, isem, wsem, ksem, vsem):
    small = [pltpu.make_async_copy(src, dst, isem.at[i]) for i, (src, dst) in enumerate((
        (x_h, x_ref), (g_h, g_ref), (lens_h, lens_ref), (freq_h, freq_ref), (bq_h, bq_ref), (bk_h, bk_ref),
        (bv_h, bv_ref), (lens_h, lens_s)))]
    later = [pltpu.make_async_copy(src, dst, isem.at[8 + i]) for i, (src, dst) in enumerate((
        (gm_h, gm_ref), (gf_h, gf_ref), (tok_h, tok_ref)))]

    def wcopy(i):
        src, dst = ((wq_h, wq), (wk_h, wk), (wv_h, wv), (wo_h, wo))[i]
        return pltpu.make_async_copy(src, dst, wsem.at[i])

    def rows(c):
        return pl.ds(pl.multiple_of(c * NB, NB), NB)

    def kin(c):
        return pltpu.make_async_copy(k_h.at[rows(c)], kbuf.at[rows(c)], ksem.at[c])

    def vin(c):
        return pltpu.make_async_copy(v_h.at[rows(c)], vbuf.at[rows(c)], vsem.at[c])

    with jax.named_scope('starts'):
        for c in small:
            c.start()
        for i in range(3):
            wcopy(i).start()
        for c in later:
            c.start()
        for c in range(AHEAD):
            kin(c).start()
            vin(c).start()

    with jax.named_scope('qkv'):
        for c in small:
            c.wait()
        normed = _rms(x_ref[...].astype(F32), _row(g_ref, D // 128))
        r_id = lax.broadcasted_iota(jnp.int32, (B, B), 0)
        c_id = lax.broadcasted_iota(jnp.int32, (B, B), 1)
        len_f = jnp.broadcast_to(lens_ref[...].astype(F32), (B, B))
        len_col = jnp.sum(jnp.where(r_id == c_id, len_f, 0.0), axis=1, keepdims=True)
        len_full = jnp.broadcast_to(len_col, (B, HD))
        len_sc[...] = len_full
        angles = len_full * freq_ref[...]
        cos = jnp.cos(angles)
        lane = lax.broadcasted_iota(jnp.int32, (B, HD), 1)
        sin = jnp.where(lane < HD // 2, -1.0, 1.0) * jnp.sin(angles)

        def rope(vals):
            out = vals * cos + pltpu.roll(vals, HD // 2, 1) * sin
            return out.astype(BF16).astype(F32)

        wcopy(0).wait()
        q_all = _dot(normed, wq[...], NN) + _row(bq_ref, G)
        for h in range(G):
            q_sc[h] = rope(q_all[:, h * HD:(h + 1) * HD])
        wcopy(1).wait()
        kn_sc[...] = rope(_dot(normed, wk[...], NN) + bk_ref[...].astype(F32))
        wcopy(2).wait()
        vn_sc[...] = (_dot(normed, wv[...], NN) + bv_ref[...].astype(F32)).astype(BF16).astype(F32)

    scale = HD ** -0.5
    sub16 = lax.broadcasted_iota(jnp.int32, (16, HD), 0)
    col_id = lax.broadcasted_iota(jnp.int32, (G * NB, L), 1).astype(F32)
    row_s = lax.broadcasted_iota(jnp.int32, (G * NB, L), 0) % NB
    row_o = lax.broadcasted_iota(jnp.int32, (G * NB, HD), 0) % NB

    def chunk(c, carry):
        r0 = pl.multiple_of(c * NB, NB)
        kin(c).wait()
        vin(c).wait()

        @pl.when(c + AHEAD < NCH)
        def _():
            kin(c + AHEAD).start()
            vin(c + AHEAD).start()

        @pl.when(c + AHEAD == NCH)
        def _():
            wcopy(3).start()

        for b in range(NB):
            row = r0 + b
            length = lens_s[0, row]
            base = pl.multiple_of((length // 16) * 16, 16)
            hit = sub16 == length - base
            for buf, new in ((kbuf, kn_sc), (vbuf, vn_sc)):
                old = buf[row, pl.ds(base, 16), :].astype(F32)
                fresh = jnp.broadcast_to(new[pl.ds(row, 1), :], (16, HD))
                buf[row, pl.ds(base, 16), :] = jnp.where(hit, fresh, old).astype(BF16)
        q8 = jnp.concatenate([q_sc[h, pl.ds(r0, NB), :] for h in range(G)], axis=0).astype(BF16)
        scores = jnp.zeros((G * NB, L), F32)
        for b in range(NB):
            scores = jnp.where(row_s == b, _dot(q8, kbuf[r0 + b], NT), scores)
        len8 = len_sc[pl.ds(r0, NB), :]
        len24 = jnp.concatenate([len8] * G, axis=0)
        keep = col_id <= jnp.concatenate([len24] * (L // HD), axis=1)
        scores = jnp.where(keep, scores * scale, -jnp.inf)
        top = jnp.max(scores, axis=1, keepdims=True)
        exps = jnp.exp(scores - top)
        probs = (exps / jnp.sum(exps, axis=1, keepdims=True)).astype(BF16)
        out = jnp.zeros((G * NB, HD), F32)
        for b in range(NB):
            out = jnp.where(row_o == b, _dot(probs, vbuf[r0 + b], NN), out)
        for h in range(G):
            o_sc[pl.ds(r0, NB), h * HD:(h + 1) * HD] = out[h * NB:(h + 1) * NB, :]
        return carry

    with jax.named_scope('cache'):
        lax.fori_loop(0, NCH, chunk, 0)
    with jax.named_scope('proj'):
        wcopy(3).wait()
        part_ref[...] = _dot(o_sc[...].astype(BF16), wo[...], NN).astype(BF16)
        for c in later:
            c.wait()


def attention(x, lens, k_cache, v_cache, g_attn, w_q, b_q, w_k, b_k, w_v, b_v, w_o, g_mlp, g_final, next_tok):
    inv_freq = np.power(THETA, np.arange(HD // 2, dtype=np.float64) * (-2.0 / HD)).astype(np.float32)
    freq = jnp.asarray(np.concatenate([inv_freq, inv_freq])[None, :])
    vmem = pl.BlockSpec(memory_space=pltpu.VMEM)
    hbm = pl.BlockSpec(memory_space=pltpu.HBM)
    return pl.pallas_call(
        attn_kernel,
        name='attn',
        out_shape=(
            pltpu.VMEM((B, D), BF16), pltpu.VMEM((B, L, HD), BF16), pltpu.VMEM((B, L, HD), BF16),
            pltpu.VMEM((B, D), BF16), pltpu.VMEM((D // 128, 128), BF16), pltpu.VMEM((D // 128, 128), BF16),
            pltpu.VMEM((1, B), jnp.int32)),
        in_specs=[hbm] * 16,
        out_specs=(vmem,) * 7,
        scratch_shapes=[
            pltpu.SMEM((1, B), jnp.int32),
            pltpu.VMEM((1, B), jnp.int32),
            pltpu.VMEM((D // 128, 128), BF16),
            pltpu.VMEM((G, 128), BF16),
            pltpu.VMEM((1, 128), BF16),
            pltpu.VMEM((1, 128), BF16),
            pltpu.VMEM((1, 128), F32),
            pltpu.VMEM((D, G * HD), BF16),
            pltpu.VMEM((D, HD), BF16),
            pltpu.VMEM((D, HD), BF16),
            pltpu.VMEM((G * HD, D), BF16),
            pltpu.VMEM((G, B, HD), F32),
            pltpu.VMEM((B, HD), F32),
            pltpu.VMEM((B, HD), F32),
            pltpu.VMEM((B, HD), F32),
            pltpu.VMEM((B, G * HD), F32),
            pltpu.SemaphoreType.DMA((11,)),
            pltpu.SemaphoreType.DMA((4,)),
            pltpu.SemaphoreType.DMA((NCH,)),
            pltpu.SemaphoreType.DMA((NCH,)),
        ],
        compiler_params=pltpu.CompilerParams(vmem_limit_bytes=8 * 1024 * 1024),
        cost_estimate=pl.CostEstimate(flops=400_000_000, bytes_accessed=37_000_000, transcendentals=0),
    )(*in_hbm(x, lens.reshape(1, B), g_attn.reshape(D // 128, 128), b_q.reshape(G, 128), b_k.reshape(1, 128),
              b_v.reshape(1, 128), freq, g_mlp.reshape(D // 128, 128), g_final.reshape(D // 128, 128),
              next_tok.reshape(1, B), w_q, w_k, w_v, w_o, k_cache, v_cache))


class Place:
    def __init__(self):
        self.dp = lax.axis_index('dp')
        self.tp = lax.axis_index('tp')
        self.core = self.tp % 2
        self.sib = self.tp + 1 - 2 * self.core
        self.xpeer = (self.tp + 2) % 4
        self.me = self.dp * NTP + self.tp
        self.ydp = self.dp + 1 - 2 * (self.dp % 2)
        self.zdp = (self.dp + 2) % 4
        self.ddp = (self.ydp + 2) % 4
        self.mine = pl.ds(pl.multiple_of(self.core * HALF, HALF), HALF)
        self.other = pl.ds(pl.multiple_of((1 - self.core) * HALF, HALF), HALF)


def _remote(send, recv):
    def make(src, dst, i, **where):
        return pltpu.make_async_remote_copy(src_ref=src, dst_ref=dst, send_sem=send.at[i], recv_sem=recv.at[i],
                                            device_id=where, device_id_type=MESH)
    return make


def sum_kernel(part_ref, x_ref, wg_h, wu_h, wd_h, a_ref, wg, wu, wd, r1, ps, r2, wsem, send, recv):
    at = Place()
    mine = at.mine
    remote = _remote(send, recv)
    loads = [pltpu.make_async_copy(src, dst, wsem.at[i]) for i, (src, dst) in enumerate((
        (wg_h, wg), (wu_h, wu), (wd_h, wd)))]
    barrier = pltpu.get_barrier_semaphore()
    pl.semaphore_signal(barrier, inc=1, device_id={'tp': at.sib}, device_id_type=MESH)
    pl.semaphore_signal(barrier, inc=1, device_id={'tp': at.xpeer}, device_id_type=MESH)
    for c in loads:
        c.start()
    with jax.named_scope('barrier1'):
        pl.semaphore_wait(barrier, 2)
    with jax.named_scope('sum1'):
        c0 = remote(part_ref.at[at.other], r1, 0, tp=at.sib)
        c0.start()
        c0.wait()
        ps[...] = (part_ref[mine, :].astype(F32) + r1[...].astype(F32)).astype(BF16)
        c1 = remote(ps, r2, 1, tp=at.xpeer)
        c1.start()
        c1.wait()
        a_ref[mine, :] = (x_ref[mine, :].astype(F32) + (ps[...].astype(F32) + r2[...].astype(F32))).astype(BF16)
        c2 = remote(a_ref.at[mine], a_ref.at[mine], 2, tp=at.sib)
        c2.start()
        c2.wait()
    with jax.named_scope('weights'):
        for c in loads:
            c.wait()


def first_sum(part, x, w_gate, w_up, w_down):
    vmem = pl.BlockSpec(memory_space=pltpu.VMEM)
    hbm = pl.BlockSpec(memory_space=pltpu.HBM)
    half = pltpu.VMEM((HALF, D), BF16)
    weight = pltpu.VMEM((FF, D), BF16)
    return pl.pallas_call(
        sum_kernel,
        name='first_sum',
        out_shape=(pltpu.VMEM((B, D), BF16), weight, weight, weight),
        in_specs=[vmem] * 2 + [hbm] * 3,
        out_specs=(vmem,) * 4,
        scratch_shapes=[
            half, half, half,
            pltpu.SemaphoreType.DMA((3,)),
            pltpu.SemaphoreType.DMA((3,)),
            pltpu.SemaphoreType.DMA((3,)),
        ],
        compiler_params=pltpu.CompilerParams(
            vmem_limit_bytes=2 * 1024 * 1024, collective_id=1, has_side_effects=True),
    )(*in_vmem(part, x), *in_hbm(w_gate.T, w_up.T, w_down))


def mlp_kernel(a_ref, wg, wu, wd, kbuf, vbuf, gm_ref, dpart, ko_h, vo_h, h_sc, ksem, vsem):
    puts = []
    for c in range(NCH):
        rows = pl.ds(c * NB, NB)
        puts.append(pltpu.make_async_copy(kbuf.at[rows], ko_h.at[rows], ksem.at[c]))
        puts.append(pltpu.make_async_copy(vbuf.at[rows], vo_h.at[rows], vsem.at[c]))
    for c in puts:
        c.start()
    with jax.named_scope('mlp'):
        mlp_in = _rms(a_ref[...].astype(F32), _row(gm_ref, D // 128))
        for s, n in FF_CHUNKS:
            gate = _dot(mlp_in, wg[s:s + n, :], NT)
            up = _dot(mlp_in, wu[s:s + n, :], NT)
            h_sc[:, s:s + n] = (gate * (1.0 / (1.0 + jnp.exp(-gate))) * up).astype(BF16)
        dpart[...] = _dot(h_sc[...], wd[...], NN).astype(BF16)
    with jax.named_scope('puts'):
        for c in puts:
            c.wait()


def mlp(a, wg, wu, wd, k_new, v_new, g_mlp):
    vmem = pl.BlockSpec(memory_space=pltpu.VMEM)
    hbm = pl.BlockSpec(memory_space=pltpu.HBM)
    cache = jax.ShapeDtypeStruct((B, L, HD), BF16)
    return pl.pallas_call(
        mlp_kernel,
        name='mlp',
        out_shape=(pltpu.VMEM((B, D), BF16), cache, cache),
        in_specs=[vmem] * 7,
        out_specs=(vmem, hbm, hbm),
        scratch_shapes=[
            pltpu.VMEM((B, FF), BF16),
            pltpu.SemaphoreType.DMA((NCH,)),
            pltpu.SemaphoreType.DMA((NCH,)),
        ],
        compiler_params=pltpu.CompilerParams(vmem_limit_bytes=8 * 1024 * 1024),
    )(*in_vmem(a, wg, wu, wd, k_new, v_new, g_mlp))


def tail_kernel(dpart, abuf, gf_ref, tok_ref, wh_h, y_ref, st_in,
                wh, r3, ps2, r4, fall, toks, st_out, hsem, send, recv, st_send, st_recv):
    at = Place()
    dp, tp, me, mine = at.dp, at.tp, at.me, at.mine
    remote = _remote(send, recv)
    v0 = dp * VQ - 8 * (dp // 3)

    def hcopy(j):
        src = wh_h.at[pl.ds(pl.multiple_of(v0 + j * VC, 8), VC)]
        return pltpu.make_async_copy(src, wh.at[pl.ds(pl.multiple_of(j * VC, VC), VC)], hsem.at[j])

    barrier = pltpu.get_barrier_semaphore()
    for k in range(1, NDP * NTP):
        there = (me + k) % (NDP * NTP)
        pl.semaphore_signal(barrier, inc=1, device_id={'dp': there // NTP, 'tp': there % NTP}, device_id_type=MESH)
    for j in range(NVC):
        hcopy(j).start()

    with jax.named_scope('barrier'):
        pl.semaphore_wait(barrier, NDP * NTP - 1)

    with jax.named_scope('sum2'):
        c3 = remote(dpart.at[at.other], r3, 3, tp=at.sib)
        c3.start()
        gain_f = _row(gf_ref, D // 128)
        toks[dp] = jnp.broadcast_to(jnp.concatenate([tok_ref[...], tok_ref[...]], axis=1), (8, 128))
        c3.wait()
        ps2[...] = (dpart[mine, :].astype(F32) + r3[...].astype(F32)).astype(BF16)
        c4 = remote(ps2, r4, 4, tp=at.xpeer)
        c4.start()
        tok_copies = [remote(toks.at[dp], toks.at[dp], 13 + i, dp=d) for i, d in enumerate((at.ydp, at.zdp, at.ddp))]
        for c in tok_copies:
            c.start()
        c4.wait()
        y_half = (abuf[mine, :].astype(F32) + (ps2[...].astype(F32) + r4[...].astype(F32))).astype(BF16)
        y_ref[mine, :] = y_half

    def frows(d, c):
        return pl.ds(pl.multiple_of(d * B + c * HALF, HALF), HALF)

    with jax.named_scope('gather'):
        own = frows(dp, at.core)
        fall[own, :] = _rms(y_half.astype(F32), gain_f)
        gathers = [remote(fall.at[own], fall.at[own], 7 + i, dp=d) for i, d in enumerate((at.ydp, at.zdp, at.ddp))]
        for c in gathers:
            c.start()
        c6 = remote(fall.at[own], fall.at[own], 6, tp=at.sib)
        c6.start()
        c5 = remote(y_ref.at[mine], y_ref.at[mine], 5, tp=at.sib)
        c5.start()
        forwards = []
        for i, d in enumerate((at.ydp, at.zdp, at.ddp)):
            gathers[i].wait_recv()
            fwd = remote(fall.at[frows(d, at.core)], fall.at[frows(d, at.core)], 10 + i, tp=at.sib)
            fwd.start()
            forwards.append(fwd)
        for c in tok_copies:
            c.wait()
        lane = lax.broadcasted_iota(jnp.int32, (8, 128), 1)
        lo = jnp.where(lane < B, toks[0], toks[1])
        hi = jnp.where(lane < B, toks[2], toks[3])
        want = jnp.concatenate([lo, hi], axis=1) - (tp * VOC + v0)
        first = 8 * (dp // 3)
        want = jnp.where((want >= first) & (want < first + VQ), want, -1)
        for c in gathers:
            c.wait_send()
        for c in forwards + [c5, c6]:
            c.wait()
        for j in range(NVC):
            hcopy(j).wait()

    sub = lax.broadcasted_iota(jnp.int32, (VC // 8, 8, NDP * B), 0) * 8 + lax.broadcasted_iota(
        jnp.int32, (VC // 8, 8, NDP * B), 1)

    def vocab(j, carry):
        top, total, target = carry
        z = _dot(wh[pl.ds(pl.multiple_of(j * VC, VC), VC), :], fall[...], NT)
        drop_first = (first > 0) & (j == 0)
        drop_last = (first == 0) & (j == NVC - 1)
        z = jnp.concatenate([
            jnp.where(drop_first, -jnp.inf, z[:8]), z[8:VC - 8], jnp.where(drop_last, -jnp.inf, z[VC - 8:])], axis=0)
        z = z.reshape(VC // 8, 8, NDP * B)
        new_top = jnp.maximum(top, jnp.max(z, axis=0))
        total = total * jnp.exp(top - new_top) + jnp.sum(jnp.exp(z - new_top[None]), axis=0)
        hit = sub == (want - j * VC)[None]
        target = target + jnp.sum(jnp.where(hit, z, 0.0), axis=0)
        return new_top, total, target

    with jax.named_scope('head'):
        def several(i, carry):
            for k in range(UNROLL):
                carry = vocab(i * UNROLL + k, carry)
            return carry

        top, total, target = lax.fori_loop(0, NVC // UNROLL, several, (
            jnp.full((8, NDP * B), -jnp.inf, F32), jnp.zeros((8, NDP * B), F32), jnp.zeros((8, NDP * B), F32)))

    with jax.named_scope('stats'):
        t_row = jnp.max(top, axis=0, keepdims=True)
        s_row = jnp.sum(total * jnp.exp(top - t_row), axis=0, keepdims=True)
        z_row = jnp.sum(target, axis=0, keepdims=True)
        row8 = lax.broadcasted_iota(jnp.int32, (8, NDP * B), 0)
        stats = jnp.where(row8 == 0, t_row, jnp.where(row8 == 1, s_row, z_row))
        st_out[0] = stats[:, :128]
        st_out[1] = stats[:, 128:]
        st_in[me] = jnp.where(dp // 2 == 0, stats[:, :128], stats[:, 128:])
        st_copies = []
        for k in range(1, NDP * NTP):
            there = (me + k) % (NDP * NTP)
            c = pltpu.make_async_remote_copy(
                src_ref=st_out.at[there // NTP // 2], dst_ref=st_in.at[me], send_sem=st_send.at[k],
                recv_sem=st_recv.at[k], device_id={'dp': there // NTP, 'tp': there % NTP}, device_id_type=MESH)
            c.start()
            st_copies.append(c)
        for c in st_copies:
            c.wait()


def finish_kernel(ybuf, stats_ref, y_ref, logp_ref, lse_ref, sem):
    put_y = pltpu.make_async_copy(ybuf, y_ref, sem.at[0])
    put_y.start()
    every = stats_ref[...]
    best = jnp.max(every[:, 0:1, :], axis=0)
    mass = jnp.sum(every[:, 1:2, :] * jnp.exp(every[:, 0:1, :] - best[None]), axis=0)
    hits = jnp.sum(every[:, 2:3, :], axis=0)
    lse = best + jnp.log(mass)
    logp = hits - lse
    left = lax.axis_index('dp') % 2 == 0
    lse_ref[...] = jnp.where(left, lse[:, :B], lse[:, B:])
    logp_ref[...] = jnp.where(left, logp[:, :B], logp[:, B:])
    put_y.wait()


def tail(dpart, a, g_final, next_tok, w_head):
    vmem = pl.BlockSpec(memory_space=pltpu.VMEM)
    hbm = pl.BlockSpec(memory_space=pltpu.HBM)
    half = pltpu.VMEM((HALF, D), BF16)
    y, stats = pl.pallas_call(
        tail_kernel,
        name='tail',
        out_shape=(pltpu.VMEM((B, D), BF16), pltpu.VMEM((NDP * NTP, 8, 128), F32)),
        in_specs=[vmem] * 4 + [hbm],
        out_specs=(vmem, vmem),
        scratch_shapes=[
            pltpu.VMEM((VC * NVC, D), BF16),
            half, half, half,
            pltpu.VMEM((NDP * B, D), BF16),
            pltpu.VMEM((NDP, 8, 128), jnp.int32),
            pltpu.VMEM((2, 8, 128), F32),
            pltpu.SemaphoreType.DMA((NVC,)),
            pltpu.SemaphoreType.DMA((16,)),
            pltpu.SemaphoreType.DMA((16,)),
            pltpu.SemaphoreType.DMA((16,)),
            pltpu.SemaphoreType.DMA((16,)),
        ],
        compiler_params=pltpu.CompilerParams(
            vmem_limit_bytes=56 * 1024 * 1024, collective_id=0, has_side_effects=True),
        cost_estimate=pl.CostEstimate(flops=10_000_000_000, bytes_accessed=50_000_000, transcendentals=0),
    )(*in_vmem(dpart, a, g_final, next_tok), *in_hbm(w_head))
    return pl.pallas_call(
        finish_kernel,
        name='finish',
        out_shape=(
            jax.ShapeDtypeStruct((B, D), BF16),
            jax.ShapeDtypeStruct((1, B), F32),
            jax.ShapeDtypeStruct((1, B), F32),
        ),
        in_specs=[vmem] * 2,
        out_specs=(hbm, vmem, vmem),
        scratch_shapes=[pltpu.SemaphoreType.DMA((1,))],
        compiler_params=pltpu.CompilerParams(vmem_limit_bytes=62 * 1024 * 1024),
    )(*in_vmem(y, stats))


def local_step(tok_hidden, seq_lens, k_cache, v_cache, next_tok, g_attn, w_q, b_q, w_k, b_k, w_v, b_v, w_o, g_mlp,
               w_gate, w_up, w_down, g_final, w_head):
    part, k_new, v_new, x, gm, gf, tok = attention(
        tok_hidden, seq_lens, k_cache.reshape(B, L, HD), v_cache.reshape(B, L, HD), g_attn, w_q, b_q, w_k, b_k, w_v,
        b_v, w_o, g_mlp, g_final, next_tok)
    a, wg, wu, wd = first_sum(part, x, w_gate, w_up, w_down)
    dpart, k_all, v_all = mlp(a, wg, wu, wd, k_new, v_new, gm)
    y_out, tok_logp, norm_lse = tail(dpart, a, gf, tok, w_head)
    return (y_out, k_all.reshape(B, L, 1, HD), v_all.reshape(B, L, 1, HD), tok_logp.reshape(B), norm_lse.reshape(B))


def solution(mesh):
    row_spec = P('dp', None)
    vec_spec = P('dp')
    cache_spec = P('dp', None, 'tp', None)
    col_spec = P(None, 'tp')
    part_spec = P('tp')
    whole_spec = P(None)
    in_specs = (row_spec, vec_spec, cache_spec, cache_spec, vec_spec, whole_spec, col_spec, part_spec, col_spec,
                part_spec, col_spec, part_spec, P('tp', None), whole_spec, col_spec, col_spec, P('tp', None),
                whole_spec, P('tp', None))
    out_specs = (row_spec, cache_spec, cache_spec, vec_spec, vec_spec)
    return jax.shard_map(local_step, mesh=mesh, in_specs=in_specs, out_specs=out_specs, check_vma=False)
```

```python
import functools
import math
import jax
import jax.numpy as jnp
import numpy as np
from jax import lax
from jax.experimental import pallas as pl
from jax.experimental.pallas import tpu as pltpu
from jax.sharding import PartitionSpec as P

THETA = 1000000.0
EPS = 1e-6
MESH = pl.DeviceIdType.MESH
F32 = jnp.float32
BF16 = jnp.bfloat16

B = 64
L = 512
D = 1536
HD = 128
G = 3
FF = 2240
VOC = 37984
NDP = 4
NTP = 4
NB = 16
NCH = B // NB
AHEAD = 2
VQ = VOC // NDP
VC = 528
NVC = 18
UNROLL = 9
KCUT = 512
HALF = B // 2
FF_CHUNKS = ((0, 512), (512, 512), (1024, 512), (1536, 512), (2048, 192))
NT = (((1,), (1,)), ((), ()))
NN = (((1,), (0,)), ((), ()))


def _dot(a, b, dims):
    return lax.dot_general(a, b, dims, preferred_element_type=F32)


def in_hbm(*arrays):
    return [pltpu.with_memory_space_constraint(a, pltpu.HBM) for a in arrays]


def in_vmem(*arrays):
    return [pltpu.with_memory_space_constraint(a, pltpu.VMEM) for a in arrays]


def _row(ref, n):
    vals = ref[...].astype(F32)
    return jnp.concatenate([vals[i:i + 1, :] for i in range(n)], axis=1)


def _rms(vals, gain):
    inv = lax.rsqrt(jnp.mean(vals * vals, axis=-1, keepdims=True) + EPS)
    return (vals * inv * gain).astype(BF16)


def attn_kernel(x_h, lens_h, g_h, bq_h, bk_h, bv_h, freq_h, gm_h, gf_h, tok_h, wq_h, wk_h, wv_h, wo_h, k_h, v_h,
                part_ref, k0, k1, k2, k3, v0, v1, v2, v3, x_ref, gm_ref, gf_ref, tok_ref,
                lens_s, lens_ref, g_ref, bq_ref, bk_ref, bv_ref, freq_ref,
                wq, wk, wv, wo, q_sc, kn_sc, vn_sc, len_sc, o_sc, isem, wsem, ksem, vsem):
    small = [pltpu.make_async_copy(src, dst, isem.at[i]) for i, (src, dst) in enumerate((
        (x_h, x_ref), (g_h, g_ref), (lens_h, lens_ref), (freq_h, freq_ref), (bq_h, bq_ref), (bk_h, bk_ref),
        (bv_h, bv_ref), (lens_h, lens_s)))]
    later = [pltpu.make_async_copy(src, dst, isem.at[8 + i]) for i, (src, dst) in enumerate((
        (gm_h, gm_ref), (gf_h, gf_ref), (tok_h, tok_ref)))]

    def wcopy(i):
        src, dst = ((wq_h, wq), (wk_h, wk), (wv_h, wv), (wo_h, wo))[i]
        return pltpu.make_async_copy(src, dst, wsem.at[i])

    kbufs = (k0, k1, k2, k3)
    vbufs = (v0, v1, v2, v3)

    def kin(c):
        return pltpu.make_async_copy(k_h.at[pl.ds(c * NB, NB)], kbufs[c], ksem.at[c])

    def vin(c):
        return pltpu.make_async_copy(v_h.at[pl.ds(c * NB, NB)], vbufs[c], vsem.at[c])

    with jax.named_scope('starts'):
        for c in small:
            c.start()
        for i in range(3):
            wcopy(i).start()
        for c in later:
            c.start()
        for c in range(AHEAD):
            kin(c).start()
            vin(c).start()

    with jax.named_scope('qkv'):
        for c in small:
            c.wait()
        normed = _rms(x_ref[...].astype(F32), _row(g_ref, D // 128))
        r_id = lax.broadcasted_iota(jnp.int32, (B, B), 0)
        c_id = lax.broadcasted_iota(jnp.int32, (B, B), 1)
        len_f = jnp.broadcast_to(lens_ref[...].astype(F32), (B, B))
        len_col = jnp.sum(jnp.where(r_id == c_id, len_f, 0.0), axis=1, keepdims=True)
        len_full = jnp.broadcast_to(len_col, (B, HD))
        len_sc[...] = len_full
        angles = len_full * freq_ref[...]
        cos = jnp.cos(angles)
        lane = lax.broadcasted_iota(jnp.int32, (B, HD), 1)
        sin = jnp.where(lane < HD // 2, -1.0, 1.0) * jnp.sin(angles)

        def rope(vals):
            out = vals * cos + pltpu.roll(vals, HD // 2, 1) * sin
            return out.astype(BF16).astype(F32)

        wcopy(0).wait()
        q_all = _dot(normed, wq[...], NN) + _row(bq_ref, G)
        for h in range(G):
            q_sc[h] = rope(q_all[:, h * HD:(h + 1) * HD])
        wcopy(1).wait()
        kn_sc[...] = rope(_dot(normed, wk[...], NN) + bk_ref[...].astype(F32))
        wcopy(2).wait()
        vn_sc[...] = (_dot(normed, wv[...], NN) + bv_ref[...].astype(F32)).astype(BF16).astype(F32)

    scale = HD ** -0.5
    ncol = G * NB
    sub16 = lax.broadcasted_iota(jnp.int32, (16, HD), 0)
    col_id = lax.broadcasted_iota(jnp.int32, (ncol, L), 1).astype(F32)
    row_q = lax.broadcasted_iota(jnp.int32, (ncol, NB * HD), 0) % NB
    blk_q = lax.broadcasted_iota(jnp.int32, (ncol, NB * HD), 1) // HD
    row_o = lax.broadcasted_iota(jnp.int32, (ncol, HD), 0) % NB

    def fresh_rows(buf, new, c):
        for b in range(NB):
            length = lens_s[0, c * NB + b]
            base = pl.multiple_of((length // 16) * 16, 16)
            old = buf[b, pl.ds(base, 16), :].astype(F32)
            row = jnp.broadcast_to(new[c * NB + b:c * NB + b + 1, :], (16, HD))
            buf[b, pl.ds(base, 16), :] = jnp.where(sub16 == length - base, row, old).astype(BF16)

    def side(buf, first, count):
        return jnp.concatenate([buf[first + b] for b in range(count)], axis=1)

    def score(c):
        heads = jnp.concatenate([q_sc[h, c * NB:(c + 1) * NB, :] for h in range(G)], axis=0)
        wide = jnp.concatenate([heads] * NB, axis=1)
        wide = jnp.where(row_q == blk_q, wide, 0.0).astype(BF16)
        return _dot(wide, side(kbufs[c], 0, NB), NT)

    def attend(c, scores):
        last = jnp.concatenate([len_sc[c * NB:(c + 1) * NB, :]] * G, axis=0)
        keep = col_id <= jnp.concatenate([last] * (L // HD), axis=1)
        scores = jnp.where(keep, scores * scale, -jnp.inf)
        exps = jnp.exp(scores - jnp.max(scores, axis=1, keepdims=True))
        probs = (exps / jnp.sum(exps, axis=1, keepdims=True)).astype(BF16)
        out = jnp.zeros((ncol, HD), F32)
        for b in range(0, NB, 2):
            both = _dot(probs, side(vbufs[c], b, 2), NN)
            out = jnp.where(row_o == b, both[:, :HD], jnp.where(row_o == b + 1, both[:, HD:], out))
        for h in range(G):
            o_sc[c * NB:(c + 1) * NB, h * HD:(h + 1) * HD] = out[h * NB:(h + 1) * NB, :]

    with jax.named_scope('cache'):
        scores = None
        for c in range(NCH):
            kin(c).wait()
            vin(c).wait()
            if c + AHEAD < NCH:
                kin(c + AHEAD).start()
                vin(c + AHEAD).start()
            if c + AHEAD == NCH:
                wcopy(3).start()
            fresh_rows(kbufs[c], kn_sc, c)
            fresh_rows(vbufs[c], vn_sc, c)
            fresh_scores = score(c)
            if c > 0:
                attend(c - 1, scores)
            scores = fresh_scores
        attend(NCH - 1, scores)
    with jax.named_scope('proj'):
        wcopy(3).wait()
        part_ref[...] = _dot(o_sc[...].astype(BF16), wo[...], NN).astype(BF16)
        for c in later:
            c.wait()


def attention(x, lens, k_cache, v_cache, g_attn, w_q, b_q, w_k, b_k, w_v, b_v, w_o, g_mlp, g_final, next_tok):
    inv_freq = np.power(THETA, np.arange(HD // 2, dtype=np.float64) * (-2.0 / HD)).astype(np.float32)
    freq = jnp.asarray(np.concatenate([inv_freq, inv_freq])[None, :])
    vmem = pl.BlockSpec(memory_space=pltpu.VMEM)
    hbm = pl.BlockSpec(memory_space=pltpu.HBM)
    return pl.pallas_call(
        attn_kernel,
        name='attn',
        out_shape=(
            pltpu.VMEM((B, D), BF16), *[pltpu.VMEM((NB, L, HD), BF16)] * (2 * NCH), pltpu.VMEM((B, D), BF16),
            pltpu.VMEM((D // 128, 128), BF16), pltpu.VMEM((D // 128, 128), BF16), pltpu.VMEM((1, B), jnp.int32)),
        in_specs=[hbm] * 16,
        out_specs=(vmem,) * (5 + 2 * NCH),
        scratch_shapes=[
            pltpu.SMEM((1, B), jnp.int32),
            pltpu.VMEM((1, B), jnp.int32),
            pltpu.VMEM((D // 128, 128), BF16),
            pltpu.VMEM((G, 128), BF16),
            pltpu.VMEM((1, 128), BF16),
            pltpu.VMEM((1, 128), BF16),
            pltpu.VMEM((1, 128), F32),
            pltpu.VMEM((D, G * HD), BF16),
            pltpu.VMEM((D, HD), BF16),
            pltpu.VMEM((D, HD), BF16),
            pltpu.VMEM((G * HD, D), BF16),
            pltpu.VMEM((G, B, HD), F32),
            pltpu.VMEM((B, HD), F32),
            pltpu.VMEM((B, HD), F32),
            pltpu.VMEM((B, HD), F32),
            pltpu.VMEM((B, G * HD), F32),
            pltpu.SemaphoreType.DMA((11,)),
            pltpu.SemaphoreType.DMA((4,)),
            pltpu.SemaphoreType.DMA((NCH,)),
            pltpu.SemaphoreType.DMA((NCH,)),
        ],
        compiler_params=pltpu.CompilerParams(vmem_limit_bytes=16 * 1024 * 1024),
        cost_estimate=pl.CostEstimate(flops=400_000_000, bytes_accessed=37_000_000, transcendentals=0),
    )(*in_hbm(x, lens.reshape(1, B), g_attn.reshape(D // 128, 128), b_q.reshape(G, 128), b_k.reshape(1, 128),
              b_v.reshape(1, 128), freq, g_mlp.reshape(D // 128, 128), g_final.reshape(D // 128, 128),
              next_tok.reshape(1, B), w_q, w_k, w_v, w_o, k_cache, v_cache))


class Place:
    def __init__(self):
        self.dp = lax.axis_index('dp')
        self.tp = lax.axis_index('tp')
        self.core = self.tp % 2
        self.sib = self.tp + 1 - 2 * self.core
        self.xpeer = (self.tp + 2) % 4
        self.me = self.dp * NTP + self.tp
        self.ydp = self.dp + 1 - 2 * (self.dp % 2)
        self.zdp = (self.dp + 2) % 4
        self.ddp = (self.ydp + 2) % 4
        self.mine = pl.ds(pl.multiple_of(self.core * HALF, HALF), HALF)
        self.other = pl.ds(pl.multiple_of((1 - self.core) * HALF, HALF), HALF)


def _remote(send, recv):
    def make(src, dst, i, **where):
        return pltpu.make_async_remote_copy(src_ref=src, dst_ref=dst, send_sem=send.at[i], recv_sem=recv.at[i],
                                            device_id=where, device_id_type=MESH)
    return make


def sum_kernel(part_ref, x_ref, wg_h, wu_h, wd_h, a_ref, wg, wu, wd, r1, ps, r2, wsem, send, recv):
    at = Place()
    mine = at.mine
    remote = _remote(send, recv)
    loads = [pltpu.make_async_copy(src, dst, wsem.at[i]) for i, (src, dst) in enumerate((
        (wg_h, wg), (wu_h, wu), (wd_h, wd)))]
    barrier = pltpu.get_barrier_semaphore()
    pl.semaphore_signal(barrier, inc=1, device_id={'tp': at.sib}, device_id_type=MESH)
    pl.semaphore_signal(barrier, inc=1, device_id={'tp': at.xpeer}, device_id_type=MESH)
    for c in loads:
        c.start()
    with jax.named_scope('barrier1'):
        pl.semaphore_wait(barrier, 2)
    with jax.named_scope('sum1'):
        c0 = remote(part_ref.at[at.other], r1, 0, tp=at.sib)
        c0.start()
        c0.wait()
        ps[...] = (part_ref[mine, :].astype(F32) + r1[...].astype(F32)).astype(BF16)
        c1 = remote(ps, r2, 1, tp=at.xpeer)
        c1.start()
        c1.wait()
        a_ref[mine, :] = (x_ref[mine, :].astype(F32) + (ps[...].astype(F32) + r2[...].astype(F32))).astype(BF16)
        c2 = remote(a_ref.at[mine], a_ref.at[mine], 2, tp=at.sib)
        c2.start()
        c2.wait()
    with jax.named_scope('weights'):
        for c in loads:
            c.wait()


def first_sum(part, x, w_gate, w_up, w_down):
    vmem = pl.BlockSpec(memory_space=pltpu.VMEM)
    hbm = pl.BlockSpec(memory_space=pltpu.HBM)
    half = pltpu.VMEM((HALF, D), BF16)
    weight = pltpu.VMEM((FF, D), BF16)
    return pl.pallas_call(
        sum_kernel,
        name='first_sum',
        out_shape=(pltpu.VMEM((B, D), BF16), weight, weight, weight),
        in_specs=[vmem] * 2 + [hbm] * 3,
        out_specs=(vmem,) * 4,
        scratch_shapes=[
            half, half, half,
            pltpu.SemaphoreType.DMA((3,)),
            pltpu.SemaphoreType.DMA((3,)),
            pltpu.SemaphoreType.DMA((3,)),
        ],
        compiler_params=pltpu.CompilerParams(
            vmem_limit_bytes=2 * 1024 * 1024, collective_id=1, has_side_effects=True),
    )(*in_vmem(part, x), *in_hbm(w_gate.T, w_up.T, w_down))


def mlp_kernel(a_ref, wg, wu, wd, gm_ref, k0, k1, k2, k3, v0, v1, v2, v3, dpart, ko_h, vo_h, h_sc, ksem, vsem):
    puts = []
    for c, (k, v) in enumerate(((k0, v0), (k1, v1), (k2, v2), (k3, v3))):
        rows = pl.ds(c * NB, NB)
        puts.append(pltpu.make_async_copy(k, ko_h.at[rows], ksem.at[c]))
        puts.append(pltpu.make_async_copy(v, vo_h.at[rows], vsem.at[c]))

    def start(_, carry):
        for c in puts:
            c.start()
        return carry

    def finish(_, carry):
        for c in puts:
            c.wait()
        return carry

    once = lax.axis_index('tp') // NTP + 1
    lax.fori_loop(0, once, start, 0)
    with jax.named_scope('mlp'):
        mlp_in = _rms(a_ref[...].astype(F32), _row(gm_ref, D // 128))
        for s, n in FF_CHUNKS:
            gate = _dot(mlp_in, wg[s:s + n, :], NT)
            up = _dot(mlp_in, wu[s:s + n, :], NT)
            h_sc[:, s:s + n] = (gate * (1.0 / (1.0 + jnp.exp(-gate))) * up).astype(BF16)
        dpart[...] = _dot(h_sc[...], wd[...], NN).astype(BF16)
    with jax.named_scope('puts'):
        lax.fori_loop(0, once, finish, 0)


def mlp(a, wg, wu, wd, g_mlp, caches):
    vmem = pl.BlockSpec(memory_space=pltpu.VMEM)
    hbm = pl.BlockSpec(memory_space=pltpu.HBM)
    cache = jax.ShapeDtypeStruct((B, L, HD), BF16)
    return pl.pallas_call(
        mlp_kernel,
        name='mlp',
        out_shape=(pltpu.VMEM((B, D), BF16), cache, cache),
        in_specs=[vmem] * (5 + 2 * NCH),
        out_specs=(vmem, hbm, hbm),
        scratch_shapes=[
            pltpu.VMEM((B, FF), BF16),
            pltpu.SemaphoreType.DMA((NCH,)),
            pltpu.SemaphoreType.DMA((NCH,)),
        ],
        compiler_params=pltpu.CompilerParams(vmem_limit_bytes=8 * 1024 * 1024),
    )(*in_vmem(a, wg, wu, wd, g_mlp, *caches))


def tail_kernel(dpart, abuf, gf_ref, tok_ref, wh_h, y_ref, st_in,
                wh, r3, ps2, r4, f0, f1, zbuf, toks, st_out, hsem, send, recv, st_send, st_recv):
    at = Place()
    dp, tp, me, mine = at.dp, at.tp, at.me, at.mine
    remote = _remote(send, recv)
    v0 = dp * VQ - 8 * (dp // 3)

    def hcopy(j):
        src = wh_h.at[pl.ds(pl.multiple_of(v0 + j * VC, 8), VC)]
        return pltpu.make_async_copy(src, wh.at[pl.ds(pl.multiple_of(j * VC, VC), VC)], hsem.at[j])

    barrier = pltpu.get_barrier_semaphore()
    for k in range(1, NDP * NTP):
        there = (me + k) % (NDP * NTP)
        pl.semaphore_signal(barrier, inc=1, device_id={'dp': there // NTP, 'tp': there % NTP}, device_id_type=MESH)
    for j in range(NVC):
        hcopy(j).start()

    with jax.named_scope('barrier'):
        pl.semaphore_wait(barrier, NDP * NTP - 1)

    with jax.named_scope('sum2'):
        c3 = remote(dpart.at[at.other], r3, 3, tp=at.sib)
        c3.start()
        gain_f = _row(gf_ref, D // 128)
        toks[dp] = jnp.broadcast_to(jnp.concatenate([tok_ref[...], tok_ref[...]], axis=1), (8, 128))
        c3.wait()
        ps2[...] = (dpart[mine, :].astype(F32) + r3[...].astype(F32)).astype(BF16)
        c4 = remote(ps2, r4, 4, tp=at.xpeer)
        c4.start()
        tok_copies = [remote(toks.at[dp], toks.at[dp], 19 + i, dp=d) for i, d in enumerate((at.ydp, at.zdp, at.ddp))]
        for c in tok_copies:
            c.start()
        c4.wait()
        y_half = (abuf[mine, :].astype(F32) + (ps2[...].astype(F32) + r4[...].astype(F32))).astype(BF16)
        y_ref[mine, :] = y_half

    def frows(d, c):
        return pl.ds(pl.multiple_of(d * B + c * HALF, HALF), HALF)

    with jax.named_scope('gather'):
        own = frows(dp, at.core)
        f_half = _rms(y_half.astype(F32), gain_f)
        f0[own, :] = f_half[:, :KCUT]
        f1[own, :] = f_half[:, KCUT:]
        peers = (at.ydp, at.zdp, at.ddp)
        gathers = [[remote(f.at[own], f.at[own], 7 + 3 * k + i, dp=d) for i, d in enumerate(peers)]
                   for k, f in enumerate((f0, f1))]
        passes = [[remote(f.at[frows(d, at.core)], f.at[frows(d, at.core)], 13 + 3 * k + i, tp=at.sib)
                   for i, d in enumerate(peers)] for k, f in enumerate((f0, f1))]
        keeps = [remote(f.at[own], f.at[own], 5 + k, tp=at.sib) for k, f in enumerate((f0, f1))]
        c5 = remote(y_ref.at[mine], y_ref.at[mine], 2, tp=at.sib)
        for c in gathers[0] + [keeps[0]] + gathers[1] + [keeps[1], c5]:
            c.start()
        for i in range(3):
            gathers[0][i].wait_recv()
            passes[0][i].start()
        for c in tok_copies:
            c.wait()
        lane = lax.broadcasted_iota(jnp.int32, (8, 128), 1)
        lo = jnp.where(lane < B, toks[0], toks[1])
        hi = jnp.where(lane < B, toks[2], toks[3])
        want = jnp.concatenate([lo, hi], axis=1) - (tp * VOC + v0)
        first = 8 * (dp // 3)
        want = jnp.where((want >= first) & (want < first + VQ), want, -1)
        for j in range(NVC):
            hcopy(j).wait()
        for c in passes[0] + [keeps[0]]:
            c.wait_recv()

    sub = lax.broadcasted_iota(jnp.int32, (VC // 8, 8, NDP * B), 0) * 8 + lax.broadcasted_iota(
        jnp.int32, (VC // 8, 8, NDP * B), 1)

    def vocab(j, carry):
        top, total, target = carry
        part = pl.ds(pl.multiple_of(j * VC, VC), VC)
        z = zbuf[part, :] + _dot(wh[part, KCUT:], f1[...], NT)
        drop_first = (first > 0) & (j == 0)
        drop_last = (first == 0) & (j == NVC - 1)
        z = jnp.concatenate([
            jnp.where(drop_first, -jnp.inf, z[:8]), z[8:VC - 8], jnp.where(drop_last, -jnp.inf, z[VC - 8:])], axis=0)
        z = z.reshape(VC // 8, 8, NDP * B)
        new_top = jnp.maximum(top, jnp.max(z, axis=0))
        total = total * jnp.exp(top - new_top) + jnp.sum(jnp.exp(z - new_top[None]), axis=0)
        hit = sub == (want - j * VC)[None]
        target = target + jnp.sum(jnp.where(hit, z, 0.0), axis=0)
        return new_top, total, target

    def first_part(js):
        for j in js:
            part = pl.ds(j * VC, VC)
            zbuf[part, :] = _dot(wh[part, :KCUT], f0[...], NT)

    with jax.named_scope('head1'):
        first_part(range(0, 6))
        for i in range(2):
            gathers[1][i].wait_recv()
            passes[1][i].start()
        first_part(range(6, 12))
        gathers[1][2].wait_recv()
        passes[1][2].start()
        first_part(range(12, NVC))
        for c in passes[1] + [keeps[1], c5]:
            c.wait_recv()
    with jax.named_scope('head'):
        def several(i, carry):
            for k in range(UNROLL):
                carry = vocab(i * UNROLL + k, carry)
            return carry

        top, total, target = lax.fori_loop(0, NVC // UNROLL, several, (
            jnp.full((8, NDP * B), -jnp.inf, F32), jnp.zeros((8, NDP * B), F32), jnp.zeros((8, NDP * B), F32)))

    with jax.named_scope('stats'):
        t_row = jnp.max(top, axis=0, keepdims=True)
        s_row = jnp.sum(total * jnp.exp(top - t_row), axis=0, keepdims=True)
        z_row = jnp.sum(target, axis=0, keepdims=True)
        row8 = lax.broadcasted_iota(jnp.int32, (8, NDP * B), 0)
        stats = jnp.where(row8 == 0, t_row, jnp.where(row8 == 1, s_row, z_row))
        st_out[0] = stats[:, :128]
        st_out[1] = stats[:, 128:]
        st_in[me] = jnp.where(dp // 2 == 0, stats[:, :128], stats[:, 128:])
        st_copies = []
        for k in range(1, NDP * NTP):
            there = (me + k) % (NDP * NTP)
            c = pltpu.make_async_remote_copy(
                src_ref=st_out.at[there // NTP // 2], dst_ref=st_in.at[me], send_sem=st_send.at[k],
                recv_sem=st_recv.at[k], device_id={'dp': there // NTP, 'tp': there % NTP}, device_id_type=MESH)
            c.start()
            st_copies.append(c)
        for c in gathers[0] + gathers[1] + passes[0] + passes[1] + keeps + [c5]:
            c.wait_send()
        for c in st_copies:
            c.wait()


def finish_kernel(ybuf, stats_ref, y_ref, logp_ref, lse_ref, sem):
    put_y = pltpu.make_async_copy(ybuf, y_ref, sem.at[0])
    put_y.start()
    every = stats_ref[...]
    best = jnp.max(every[:, 0:1, :], axis=0)
    mass = jnp.sum(every[:, 1:2, :] * jnp.exp(every[:, 0:1, :] - best[None]), axis=0)
    hits = jnp.sum(every[:, 2:3, :], axis=0)
    lse = best + jnp.log(mass)
    logp = hits - lse
    left = lax.axis_index('dp') % 2 == 0
    lse_ref[...] = jnp.where(left, lse[:, :B], lse[:, B:])
    logp_ref[...] = jnp.where(left, logp[:, :B], logp[:, B:])
    put_y.wait()


def tail(dpart, a, g_final, next_tok, w_head):
    vmem = pl.BlockSpec(memory_space=pltpu.VMEM)
    hbm = pl.BlockSpec(memory_space=pltpu.HBM)
    half = pltpu.VMEM((HALF, D), BF16)
    y, stats = pl.pallas_call(
        tail_kernel,
        name='tail',
        out_shape=(pltpu.VMEM((B, D), BF16), pltpu.VMEM((NDP * NTP, 8, 128), F32)),
        in_specs=[vmem] * 4 + [hbm],
        out_specs=(vmem, vmem),
        scratch_shapes=[
            pltpu.VMEM((VC * NVC, D), BF16),
            half, half, half,
            pltpu.VMEM((NDP * B, KCUT), BF16),
            pltpu.VMEM((NDP * B, D - KCUT), BF16),
            pltpu.VMEM((NVC * VC, NDP * B), F32),
            pltpu.VMEM((NDP, 8, 128), jnp.int32),
            pltpu.VMEM((2, 8, 128), F32),
            pltpu.SemaphoreType.DMA((NVC,)),
            pltpu.SemaphoreType.DMA((22,)),
            pltpu.SemaphoreType.DMA((22,)),
            pltpu.SemaphoreType.DMA((16,)),
            pltpu.SemaphoreType.DMA((16,)),
        ],
        compiler_params=pltpu.CompilerParams(
            vmem_limit_bytes=56 * 1024 * 1024, collective_id=0, has_side_effects=True),
        cost_estimate=pl.CostEstimate(flops=10_000_000_000, bytes_accessed=50_000_000, transcendentals=0),
    )(*in_vmem(dpart, a, g_final, next_tok), *in_hbm(w_head))
    return pl.pallas_call(
        finish_kernel,
        name='finish',
        out_shape=(
            jax.ShapeDtypeStruct((B, D), BF16),
            jax.ShapeDtypeStruct((1, B), F32),
            jax.ShapeDtypeStruct((1, B), F32),
        ),
        in_specs=[vmem] * 2,
        out_specs=(hbm, vmem, vmem),
        scratch_shapes=[pltpu.SemaphoreType.DMA((1,))],
        compiler_params=pltpu.CompilerParams(vmem_limit_bytes=62 * 1024 * 1024),
    )(*in_vmem(y, stats))


def local_step(tok_hidden, seq_lens, k_cache, v_cache, next_tok, g_attn, w_q, b_q, w_k, b_k, w_v, b_v, w_o, g_mlp,
               w_gate, w_up, w_down, g_final, w_head):
    part, *caches, x, gm, gf, tok = attention(
        tok_hidden, seq_lens, k_cache.reshape(B, L, HD), v_cache.reshape(B, L, HD), g_attn, w_q, b_q, w_k, b_k, w_v,
        b_v, w_o, g_mlp, g_final, next_tok)
    a, wg, wu, wd = first_sum(part, x, w_gate, w_up, w_down)
    dpart, k_all, v_all = mlp(a, wg, wu, wd, gm, caches)
    y_out, tok_logp, norm_lse = tail(dpart, a, gf, tok, w_head)
    return (y_out, k_all.reshape(B, L, 1, HD), v_all.reshape(B, L, 1, HD), tok_logp.reshape(B), norm_lse.reshape(B))


def solution(mesh):
    row_spec = P('dp', None)
    vec_spec = P('dp')
    cache_spec = P('dp', None, 'tp', None)
    col_spec = P(None, 'tp')
    part_spec = P('tp')
    whole_spec = P(None)
    in_specs = (row_spec, vec_spec, cache_spec, cache_spec, vec_spec, whole_spec, col_spec, part_spec, col_spec,
                part_spec, col_spec, part_spec, P('tp', None), whole_spec, col_spec, col_spec, P('tp', None),
                whole_spec, P('tp', None))
    out_specs = (row_spec, cache_spec, cache_spec, vec_spec, vec_spec)
    return jax.shard_map(local_step, mesh=mesh, in_specs=in_specs, out_specs=out_specs, check_vma=False)
```
